128 devices in a mesh: shard: 32 (over x, z, core), task: 4 (over y).
Axes of the slice: x: 4, y: 4, z: 4, core: 2. Of those that a mesh axis runs over, the one named last changes fastest.
Arguments:
- task_deltas: bfloat16 [4, 4, 512, 16384], P('task', None, 'shard')
- rank_scores: int32 [4, 4, 512, 16384], P('task', None, 'shard'), may hold values from 0 to 1073741823
- keep_limits: int32 [4, 4, 8], P('task'), may hold values from 268435456 to 805306367
Outputs:
- merged: bfloat16 [4, 512, 16384], P(None, 'shard', 'task')
The draws below stay inside these ranges and needn't reach their ends.
All inputs are finite; a program needn't handle non-finite values.
Results may differ from the reference program's by a relative error of at most 0.0051.
Values may be sent and summed in bfloat16 or wider, within the bound.
A program may use at most 64 MiB of HBM per device.

```python
import math
import jax
import jax.numpy as jnp
from jax import lax

EXPERTS = 8
FF = 16384
LAYERS = 4
ROWS = 64
TASKS = 4


def draw_task_deltas(key, part):
    key_base, key_column, key_row = jax.random.split(key, 3)
    row_total = EXPERTS * ROWS
    shape = (TASKS, LAYERS, row_total, FF)
    rising = 1.0 + 2.0 * jnp.arange(row_total, dtype=jnp.float32) / max(row_total - 1, 1)
    base = jax.random.normal(key_base, shape, jnp.float32)
    column = 0.03 * jnp.exp(jax.random.uniform(key_column, (TASKS, LAYERS, 1, FF), jnp.float32, 0.0, math.log(10.0)))
    row_scale = jnp.exp(jax.random.uniform(key_row, (TASKS, LAYERS, row_total, 1), jnp.float32, 0.0, math.log(10.0)))
    return (base * column * row_scale * rising[None, None, :, None]).astype(jnp.bfloat16)


def plant(result, stream_key, smallest, top_value):
    longest = result.shape.index(max(result.shape))
    spots = []
    for shift in (0, 1):
        where = [jax.random.randint(jax.random.fold_in(stream_key, axis), (), 0, length) for axis, length in enumerate(result.shape)]
        where[longest] = (where[longest] + shift) % result.shape[longest]
        spots.append(tuple(where))
    return result.at[spots[0]].set(smallest).at[spots[1]].set(top_value)


def setup_inputs(seed: int = 0) -> dict:
    key_list = jax.random.split(jax.random.key(seed), 4)
    return {
        "task_deltas": draw_task_deltas(jax.random.fold_in(key_list[3], 71), 0),
        "rank_scores": plant(jax.random.randint(key_list[1], (TASKS, LAYERS, EXPERTS * ROWS, FF), 0, 1073741824), jax.random.fold_in(key_list[1], 1), 0, 1073741823).astype(jnp.int32),
        "keep_limits": plant(jax.random.randint(key_list[2], (TASKS, LAYERS, EXPERTS), 268435456, 805306368), jax.random.fold_in(key_list[2], 1), 268435456, 805306367).astype(jnp.int32),
    }


def keep_probability(column_sums, grand_sums, row_total):
    column_mean = column_sums / row_total
    grand_mean = grand_sums / (EXPERTS * row_total * FF)
    return (0.2 + 0.7 * column_mean / (column_mean + grand_mean)).astype(jnp.bfloat16)


def reference(task_deltas, rank_scores, keep_limits):
    outputs = []
    for layer_at in range(LAYERS):
        change = task_deltas[:, layer_at].astype(jnp.float32).reshape(TASKS, EXPERTS, ROWS, FF)
        column_sums = jnp.sum(jnp.abs(change), axis=2)
        grand_sums = jnp.sum(column_sums, axis=(1, 2))
        rounded = lax.optimization_barrier(keep_probability(column_sums, grand_sums[:, None, None], ROWS))
        probability = rounded.astype(jnp.float32)
        scores = rank_scores[:, layer_at].reshape(TASKS, EXPERTS, ROWS, FF)
        limits = keep_limits[:, layer_at][:, :, None, None]
        retained = jnp.where(scores < limits, change / probability[:, :, None, :], jnp.float32(0.0))
        merged = jnp.sum(retained, axis=0).reshape(EXPERTS * ROWS, FF).astype(jnp.bfloat16)
        outputs.append(merged)
    return jnp.stack(outputs)
```

```python
import functools

import jax
import jax.numpy as jnp
from jax import lax
from jax.experimental import pallas as pl
from jax.experimental.pallas import tpu as pltpu
from jax.sharding import PartitionSpec as P

EXPERTS = 8
ROWS = 64
FF = 16384
LAYERS = 4
TASKS = 4
SHARDS = 32
GROUP = 4
PLANE = 8
HERE = 16
HALF = 2048
LANES = 128
PARTS = HALF // LANES
RAW = 4

MESH = pl.DeviceIdType.MESH
F32 = jnp.float32
BF16 = jnp.bfloat16


def kernel(
    delta, score, limit, out,
    dbuf, sbuf, masked, sums, sums_in, prob, prob_in, inv, acc, raw_in,
    tot, tot_x, tot2, tot_z,
    sem_d, sem_s, sem_sum, sem_x, sem_z, sem_p, sem_py, sem_r, sem_o,
):
    s, t = lax.axis_index("shard"), lax.axis_index("task")
    expert = lax.div(s, GROUP)
    member = lax.rem(s, GROUP)
    first = expert * GROUP
    plane, spot = lax.div(s, PLANE) * PLANE, lax.rem(s, PLANE)

    def at_task(d):
        return (s, lax.rem(t + d, TASKS))

    def at_x(d):
        return (lax.rem(s + PLANE * d, SHARDS), t)

    def at_plane(d):
        return (plane + lax.rem(spot + d, PLANE), t)

    def at_group(d):
        return (first + lax.rem(member + d, GROUP), t)

    def send(src, dst, sems, at, to):
        copy = pltpu.make_async_remote_copy(
            src_ref=src, dst_ref=dst, send_sem=sems.at[(0, *at)], recv_sem=sems.at[(1, *at)],
            device_id=to, device_id_type=MESH,
        )
        copy.start()
        return copy

    load_d = [pltpu.make_async_copy(delta.at[0, l], dbuf.at[l], sem_d.at[l]) for l in range(LAYERS)]
    load_s = [pltpu.make_async_copy(score.at[0, l], sbuf.at[l], sem_s.at[l]) for l in range(LAYERS)]
    load_d[0].start()
    load_s[0].start()
    for l in range(1, LAYERS):
        load_d[l].start()
    for l in range(1, LAYERS):
        load_s[l].start()

    barrier = pltpu.get_barrier_semaphore()
    peers = [at_task(d) for d in (1, 2, 3)] + [at_x(d) for d in (1, 2, 3)] + [at_plane(d) for d in range(1, PLANE)]
    for peer in peers:
        pl.semaphore_signal(barrier, inc=1, device_id=peer, device_id_type=MESH)

    def sum_layer(l):
        def body(i, carry):
            b, h = lax.div(i, 2), lax.rem(i, 2)
            for j in range(PARTS):
                cols = pl.ds(pl.multiple_of(i * HALF + j * LANES, LANES), LANES)
                change = jnp.abs(dbuf[l, :, cols].astype(F32))
                sums[b, l, h, j : j + 1, :] = jnp.sum(change, axis=0, keepdims=True)
            return carry

        lax.fori_loop(0, 2 * TASKS, body, 0)

    def mask_layer(l):
        own_limit = limit[0, l, expert]

        def body(i, carry):
            b, h = lax.div(i, 2), lax.rem(i, 2)
            for j in range(PARTS):
                cols = pl.ds(pl.multiple_of(i * HALF + j * LANES, LANES), LANES)
                keep = sbuf[l, :, cols] < own_limit
                masked[b, l, h, :, j * LANES : (j + 1) * LANES] = jnp.where(
                    keep, dbuf[l, :, cols].astype(F32), F32(0.0)
                ).astype(BF16)
            return carry

        lax.fori_loop(0, 2 * TASKS, body, 0)

    copies = []

    def send_raw(l):
        for d in (1, 3, 2):
            owner = lax.rem(t + d, TASKS)
            copies.append((("raw", d, l), send(masked.at[owner, l], raw_in.at[d - 1, l], sem_r, (d - 1, l), at_task(d))))

    load_d[0].wait()
    load_s[0].wait()
    mask_layer(0)
    pl.semaphore_wait(barrier, len(peers))
    send_raw(0)
    sum_layer(0)
    for l in range(1, LAYERS):
        load_d[l].wait()
        sum_layer(l)

    for d in range(1, GROUP):
        other = lax.rem(member + d, GROUP)
        copies.append((("sum", d), send(sums.at[other], sums_in.at[d - 1], sem_sum, (d - 1,), at_group(d))))
    for l in range(LAYERS):
        whole = sums[0, l, 0] + sums[0, l, 1]
        for b in range(1, TASKS):
            whole = whole + sums[b, l, 0] + sums[b, l, 1]
        tot[l : l + 1, :] = jnp.sum(whole, axis=0, keepdims=True)
    tot[LAYERS:, :] = jnp.zeros((8 - LAYERS, LANES), F32)
    for d in (1, 2, 3):
        copies.append((("x", d), send(tot, tot_x.at[d - 1], sem_x, (d - 1,), at_x(d))))

    for l in range(1, LAYERS):
        load_s[l].wait()
        mask_layer(l)
        send_raw(l)

    flight = dict(copies)
    for d in (1, 2, 3):
        flight["x", d].wait_recv()
    tot2[...] = tot[...] + tot_x[0] + tot_x[1] + tot_x[2]
    for d in range(1, PLANE):
        flight["z", d] = send(tot2, tot_z.at[d - 1], sem_z, (d - 1,), at_plane(d))
    for d in range(1, GROUP):
        flight["sum", d].wait_recv()
    for d in range(1, PLANE):
        flight["z", d].wait_recv()
    grand = tot2[...]
    for d in range(1, PLANE):
        grand = grand + tot_z[d - 1]
    grand_mean = jnp.sum(grand, axis=1, keepdims=True) / F32(EXPERTS * ROWS * FF)

    for l in range(LAYERS):
        mean_l = jnp.broadcast_to(grand_mean[l : l + 1, :], (PARTS, LANES))
        for h in range(2):
            column = sums[member, l, h] + sums_in[0, l, h] + sums_in[1, l, h] + sums_in[2, l, h]
            column = column / F32(ROWS)
            prob[member, l, h] = (0.2 + 0.7 * column / (column + mean_l)).astype(BF16)
    for d in range(1, GROUP):
        flight["p", d] = send(prob.at[member], prob.at[member], sem_p, (d - 1,), at_group(d))
    for d in range(1, GROUP):
        flight["p", d].wait_recv()
    for d in (1, 3, 2):
        owner = lax.rem(t + d, TASKS)
        flight["py", d] = send(prob.at[owner], prob_in.at[d - 1], sem_py, (d - 1,), at_task(d))

    def rescaled(block, tile, j):
        return block[:, j * LANES : (j + 1) * LANES].astype(F32) * tile[j : j + 1, :]

    for l in range(LAYERS):
        for h in range(2):
            tile = 1.0 / prob[t, l, h].astype(F32)
            block = masked.at[t, l, h]
            for j in range(PARTS):
                acc[l, h, :, j * LANES : (j + 1) * LANES] = rescaled(block, tile, j)
    for d in (1, 3, 2):
        flight["py", d].wait_recv()
    for d in (1, 2, 3):
        for l in range(LAYERS):
            for h in range(2):
                inv[d - 1, l, h] = 1.0 / prob_in[d - 1, l, h].astype(F32)
    store = []
    for l in range(LAYERS):
        for d in (1, 3, 2):
            flight["raw", d, l].wait_recv()
        for h in range(2):
            tiles = [inv[d, l, h] for d in range(3)]
            for j in range(PARTS):
                here = acc[l, h, :, j * LANES : (j + 1) * LANES]
                for d in range(3):
                    here = here + rescaled(raw_in.at[d, l, h], tiles[d], j)
                out[l, :, h * HALF + j * LANES : h * HALF + (j + 1) * LANES] = here.astype(BF16)
    for copy in flight.values():
        copy.wait_send()


def on_device(task_deltas, rank_scores, keep_limits):
    dma = pltpu.SemaphoreType.DMA
    return pl.pallas_call(
        kernel,
        out_shape=jax.ShapeDtypeStruct((LAYERS, HERE, 2 * HALF), BF16),
        in_specs=[
            pl.BlockSpec(memory_space=pl.ANY),
            pl.BlockSpec(memory_space=pl.ANY),
            pl.BlockSpec(memory_space=pltpu.SMEM),
        ],
        out_specs=pl.BlockSpec(memory_space=pltpu.VMEM),
        scratch_shapes=[
            pltpu.VMEM((LAYERS, HERE, FF), BF16),
            pltpu.VMEM((LAYERS, HERE, FF), jnp.int32),
            pltpu.VMEM((TASKS, LAYERS, 2, HERE, HALF), BF16),
            pltpu.VMEM((TASKS, LAYERS, 2, PARTS, LANES), F32),
            pltpu.VMEM((3, LAYERS, 2, PARTS, LANES), F32),
            pltpu.VMEM((TASKS, LAYERS, 2, PARTS, LANES), BF16),
            pltpu.VMEM((3, LAYERS, 2, PARTS, LANES), BF16),
            pltpu.VMEM((3, LAYERS, 2, PARTS, LANES), F32),
            pltpu.VMEM((LAYERS, 2, HERE, HALF), F32),
            pltpu.VMEM((3, LAYERS, 2, HERE, HALF), BF16),
            pltpu.VMEM((8, LANES), F32),
            pltpu.VMEM((3, 8, LANES), F32),
            pltpu.VMEM((8, LANES), F32),
            pltpu.VMEM((PLANE - 1, 8, LANES), F32),
            dma((LAYERS,)),
            dma((LAYERS,)),
            dma((2, 3)),
            dma((2, 3)),
            dma((2, PLANE - 1)),
            dma((2, 3)),
            dma((2, 3)),
            dma((2, 3, LAYERS)),
            dma((LAYERS,)),
        ],
        compiler_params=pltpu.CompilerParams(collective_id=0, has_side_effects=True),
    )(task_deltas, rank_scores, keep_limits)


def solution(mesh):
    in_specs = (P("task", None, "shard", None), P("task", None, "shard", None), P("task", None, None))
    return jax.shard_map(on_device, mesh=mesh, in_specs=in_specs, out_specs=P(None, "shard", "task"), check_vma=False)
```

```python
import functools

import jax
import jax.numpy as jnp
from jax import lax
from jax.experimental import pallas as pl
from jax.experimental.pallas import tpu as pltpu
from jax.sharding import PartitionSpec as P

EXPERTS = 8
ROWS = 64
FF = 16384
LAYERS = 4
TASKS = 4
SHARDS = 32
GROUP = 4
HERE = 16
HALF = 2048
LANES = 128
PARTS = HALF // LANES
RAW = 2
REST = LAYERS - RAW

MESH = pl.DeviceIdType.MESH
F32 = jnp.float32
BF16 = jnp.bfloat16


def kernel(
    delta, score, limit_in, out,
    limit, dbuf, sbuf, masked, sums, sums_in, prob, prob_in, inv, acc, raw_in,
    far, far_in, joint, joint_in, tot, tot_z, tot2, tot_x, grand,
    sem_load, sem_sent, sem_got, sem_f, sem_j,
):
    s, t = lax.axis_index("shard"), lax.axis_index("task")
    expert = lax.div(s, GROUP)
    member = lax.rem(s, GROUP)
    first = expert * GROUP
    late = lax.rem(expert, 2)
    hub = (expert - late) * GROUP
    other = hub + (1 - late) * GROUP

    def at_task(d):
        return (s, lax.rem(t + d, TASKS))

    def at_x(d):
        return (lax.rem(s + 2 * GROUP * d, SHARDS), t)

    def at_group(d):
        return (first + lax.rem(member + d, GROUP), t)

    def send(src, dst, kind, to, got=None):
        copy = pltpu.make_async_remote_copy(
            src_ref=src, dst_ref=dst, send_sem=sem_sent.at[kind], recv_sem=sem_got.at[kind] if got is None else got,
            device_id=to, device_id_type=MESH,
        )
        copy.start()
        return copy

    def wait(ref, sem):
        pltpu.make_async_copy(ref, ref, sem).wait()

    def shares(ref):
        return {0: ref.at[pl.ds(0, 1)], 1: ref.at[:, pl.ds(0, 2)], 2: ref.at[pl.ds(0, 2)], 4: ref}[RAW]

    SUM, TOTAL, TOTAL_X, GRAND, PROB, PROB_Y, ENTRY, FAR, JOINT = range(9)

    barrier = pltpu.get_barrier_semaphore()

    def greet(to):
        pl.semaphore_signal(barrier, inc=1, device_id=to, device_id_type=MESH)

    for d in (1, 2, 3):
        greet(at_task(d))
        greet(at_group(d))

    @pl.when(late == 0)
    def _():
        for d in (1, 2, 3):
            greet(at_x(d))
        for m in range(GROUP):
            greet((other + m, t))

    loads = [
        pltpu.make_async_copy(limit_in, limit, sem_load.at[0]),
        pltpu.make_async_copy(delta.at[0, 0], dbuf.at[0], sem_load.at[1]),
        pltpu.make_async_copy(score.at[0, 0], sbuf.at[0], sem_load.at[2]),
        pltpu.make_async_copy(delta.at[0, pl.ds(1, LAYERS - 1)], dbuf.at[pl.ds(1, LAYERS - 1)], sem_load.at[3]),
        pltpu.make_async_copy(score.at[0, pl.ds(1, LAYERS - 1)], sbuf.at[pl.ds(1, LAYERS - 1)], sem_load.at[4]),
    ]
    for load in loads:
        load.start()

    def sum_layer(l):
        def body(i, carry):
            b, h = lax.div(i, 2), lax.rem(i, 2)
            for j in range(PARTS):
                cols = pl.ds(pl.multiple_of(i * HALF + j * LANES, LANES), LANES)
                change = jnp.abs(dbuf[l, :, cols].astype(F32))
                sums[b, l, h, j : j + 1, :] = jnp.sum(change, axis=0, keepdims=True)
            return carry

        lax.fori_loop(0, 2 * TASKS, body, 0)

    def mask_layer(l):
        own_limit = limit[0, l, expert]

        def body(i, carry):
            b, h = lax.div(i, 2), lax.rem(i, 2)
            for j in range(PARTS):
                cols = pl.ds(pl.multiple_of(i * HALF + j * LANES, LANES), LANES)
                keep = sbuf[l, :, cols] < own_limit
                masked[b, l, h, :, j * LANES : (j + 1) * LANES] = jnp.where(
                    keep, dbuf[l, :, cols].astype(F32), F32(0.0)
                ).astype(BF16)
            return carry

        lax.fori_loop(0, 2 * TASKS, body, 0)

    flight = []

    def send_raw(l):
        for d in (1, 3, 2) if l < RAW else (1, 3):
            owner = lax.rem(t + d, TASKS)
            if l < RAW:
                flight.append(send(masked.at[owner, l], raw_in.at[d - 1, l], ENTRY, at_task(d)))
            else:
                h = 1 if d == 1 else 0
                flight.append(send(masked.at[owner, l, h], raw_in.at[d - 1, l, h], ENTRY, at_task(d)))

    with jax.named_scope("load"):
        for load in loads[:3]:
            load.wait()
    with jax.named_scope("mask0"):
        mask_layer(0)
    with jax.named_scope("bar"):
        pl.semaphore_wait(barrier, 9 + late)
    send_raw(0)
    with jax.named_scope("sums"):
        sum_layer(0)
        loads[3].wait()
        for l in range(1, LAYERS):
            sum_layer(l)

    for l in range(LAYERS):
        whole = sums[0, l, 0] + sums[0, l, 1]
        for b in range(1, TASKS):
            whole = whole + sums[b, l, 0] + sums[b, l, 1]
        tot[l : l + 1, :] = jnp.sum(whole, axis=0, keepdims=True)
    tot[LAYERS:, :] = jnp.zeros((8 - LAYERS, LANES), F32)

    @pl.when(late == 0)
    def _():
        for d in range(1, GROUP):
            send(tot, tot_z.at[d - 1], TOTAL, at_group(d))

    @pl.when(late == 1)
    def _():
        for m in range(GROUP):
            send(tot, tot_z.at[GROUP - 1 + member], TOTAL, (other + m, t))

    for d in range(1, GROUP):
        send(sums.at[lax.rem(member + d, GROUP)], sums_in.at[d - 1], SUM, at_group(d))

    with jax.named_scope("masks"):
        loads[4].wait()
        for l in range(1, LAYERS):
            mask_layer(l)
            send_raw(l)

    with jax.named_scope("totals"):

        @pl.when(late == 0)
        def _():
            wait(tot_z, sem_got.at[TOTAL])
            whole = tot[...]
            for d in range(2 * GROUP - 1):
                whole = whole + tot_z[d]
            tot2[...] = whole
            for d in (1, 2, 3):
                send(tot2, tot_x.at[d - 1], TOTAL_X, at_x(d))
            wait(tot_x, sem_got.at[TOTAL_X])
            grand[...] = tot2[...] + tot_x[0] + tot_x[1] + tot_x[2]
            send(grand, grand, GRAND, (other + member, t))

        @pl.when(late == 1)
        def _():
            wait(grand, sem_got.at[GRAND])

    grand_mean = jnp.sum(grand[...], axis=1, keepdims=True) / F32(EXPERTS * ROWS * FF)
    with jax.named_scope("waitsum"):
        wait(sums_in, sem_got.at[SUM])

    for l in range(LAYERS):
        mean_l = jnp.broadcast_to(grand_mean[l : l + 1, :], (PARTS, LANES))
        for h in range(2):
            column = sums[member, l, h] + sums_in[0, l, h] + sums_in[1, l, h] + sums_in[2, l, h]
            column = column / F32(ROWS)
            prob[member, l, h] = (0.2 + 0.7 * column / (column + mean_l)).astype(BF16)
    for d in range(1, GROUP):
        send(prob.at[member], prob.at[member], PROB, at_group(d))
    with jax.named_scope("waitp"):
        wait(prob.at[pl.ds(0, GROUP - 1)], sem_got.at[PROB])

    def rescaled(block, tile, j):
        return block[:, j * LANES : (j + 1) * LANES].astype(F32) * tile[j : j + 1, :]

    far_owner = lax.rem(t + 2, TASKS)
    with jax.named_scope("far"):
        for l in range(RAW, LAYERS):
            for h in range(2):
                tile = 1.0 / prob[far_owner, l, h].astype(F32)
                for j in range(PARTS):
                    far[h, l - RAW, :, j * LANES : (j + 1) * LANES] = rescaled(
                        masked.at[far_owner, l, h], tile, j
                    ).astype(BF16)
                flight.append(
                    send(far.at[h, l - RAW], far_in.at[h, l - RAW], FAR, at_task(3 if h else 1), sem_f.at[h, l - RAW])
                )
    for d in (1, 3):
        owner, h = lax.rem(t + d, TASKS), 1 if d == 1 else 0
        if RAW < LAYERS:
            rest = pl.ds(RAW, LAYERS - RAW)
            send(prob.at[owner, rest, h], prob_in.at[d - 1, rest, h], PROB_Y, at_task(d))
    for d in (1, 3, 2) if RAW else ():
        some = pl.ds(0, RAW)
        send(prob.at[lax.rem(t + d, TASKS), some], prob_in.at[d - 1, some], PROB_Y, at_task(d))

    with jax.named_scope("own"):
        for l in range(LAYERS):
            for h in range(2):
                tile = 1.0 / prob[t, l, h].astype(F32)
                for j in range(PARTS):
                    acc[l, h, :, j * LANES : (j + 1) * LANES] = rescaled(masked.at[t, l, h], tile, j)

    for l in range(RAW, LAYERS):
        for h in range(2):
            with jax.named_scope(f"waitfar#l={l}#h={h}"):
                wait(far_in.at[h, l - RAW], sem_f.at[h, l - RAW])
            owner = lax.rem(t + (3 if h else 1), TASKS)
            tile = 1.0 / prob[owner, l, h].astype(F32)
            for j in range(PARTS):
                cols = slice(j * LANES, (j + 1) * LANES)
                joint[h, l - RAW, :, cols] = (
                    rescaled(masked.at[owner, l, h], tile, j) + far_in[h, l - RAW, :, cols].astype(F32)
                ).astype(BF16)
            send(joint.at[h, l - RAW], joint_in.at[h, l - RAW], JOINT, at_task(3 if h else 1), sem_j.at[h, l - RAW])

    with jax.named_scope("waitpy"):
        wait(shares(prob_in), sem_got.at[PROB_Y])
    for d in (1, 2, 3):
        for l in range(LAYERS):
            for h in range(2):
                if l < RAW or (d, h) in ((1, 1), (3, 0)):
                    inv[d - 1, l, h] = 1.0 / prob_in[d - 1, l, h].astype(F32)
    with jax.named_scope("waitraw"):
        wait(shares(raw_in), sem_got.at[ENTRY])
    with jax.named_scope("raw"):
        for l in range(LAYERS):
            for h in range(2):
                sources = (1, 2, 3) if l < RAW else (1,) if h else (3,)
                tiles = {d: inv[d - 1, l, h] for d in sources}
                for j in range(PARTS):
                    cols = slice(j * LANES, (j + 1) * LANES)
                    here = acc[l, h, :, cols]
                    for d in sources:
                        here = here + rescaled(raw_in.at[d - 1, l, h], tiles[d], j)
                    if l < RAW:
                        out[l, :, h * HALF + j * LANES : h * HALF + (j + 1) * LANES] = here.astype(BF16)
                    else:
                        acc[l, h, :, cols] = here
    for l in range(RAW, LAYERS):
        for h in range(2):
            with jax.named_scope(f"waitjoint#l={l}#h={h}"):
                wait(joint_in.at[h, l - RAW], sem_j.at[h, l - RAW])
            for j in range(PARTS):
                cols = slice(j * LANES, (j + 1) * LANES)
                out[l, :, h * HALF + j * LANES : h * HALF + (j + 1) * LANES] = (
                    acc[l, h, :, cols] + joint_in[h, l - RAW, :, cols].astype(F32)
                ).astype(BF16)

    with jax.named_scope("waitsend"):

        @pl.when(late == 0)
        def _():
            wait(tot_z.at[pl.ds(0, GROUP - 1)], sem_sent.at[TOTAL])
            wait(tot_x, sem_sent.at[TOTAL_X])
            wait(grand, sem_sent.at[GRAND])

        @pl.when(late == 1)
        def _():
            wait(tot_z.at[pl.ds(0, GROUP)], sem_sent.at[TOTAL])

        wait(sums_in, sem_sent.at[SUM])
        wait(prob.at[pl.ds(0, GROUP - 1)], sem_sent.at[PROB])
        wait(shares(prob_in), sem_sent.at[PROB_Y])
        wait(shares(raw_in), sem_sent.at[ENTRY])
        if RAW < LAYERS:
            wait(far, sem_sent.at[FAR])
            wait(joint, sem_sent.at[JOINT])


def on_device(task_deltas, rank_scores, keep_limits):
    dma = pltpu.SemaphoreType.DMA
    inputs = (pltpu.with_memory_space_constraint(x, pltpu.HBM) for x in (task_deltas, rank_scores, keep_limits))
    return pl.pallas_call(
        kernel,
        out_shape=jax.ShapeDtypeStruct((LAYERS, HERE, 2 * HALF), BF16),
        in_specs=[pl.BlockSpec(memory_space=pl.ANY)] * 3,
        out_specs=pl.BlockSpec(memory_space=pltpu.VMEM),
        scratch_shapes=[
            pltpu.SMEM((1, LAYERS, EXPERTS), jnp.int32),
            pltpu.VMEM((LAYERS, HERE, FF), BF16),
            pltpu.VMEM((LAYERS, HERE, FF), jnp.int32),
            pltpu.VMEM((TASKS, LAYERS, 2, HERE, HALF), BF16),
            pltpu.VMEM((TASKS, LAYERS, 2, PARTS, LANES), F32),
            pltpu.VMEM((GROUP - 1, LAYERS, 2, PARTS, LANES), F32),
            pltpu.VMEM((TASKS, LAYERS, 2, PARTS, LANES), BF16),
            pltpu.VMEM((3, LAYERS, 2, PARTS, LANES), BF16),
            pltpu.VMEM((3, LAYERS, 2, PARTS, LANES), F32),
            pltpu.VMEM((LAYERS, 2, HERE, HALF), F32),
            pltpu.VMEM((3, LAYERS, 2, HERE, HALF), BF16),
            *[pltpu.VMEM((2, REST, HERE, HALF), BF16)] * 4,
            pltpu.VMEM((8, LANES), F32),
            pltpu.VMEM((2 * GROUP - 1, 8, LANES), F32),
            pltpu.VMEM((8, LANES), F32),
            pltpu.VMEM((3, 8, LANES), F32),
            pltpu.VMEM((8, LANES), F32),
            dma((5,)),
            dma((9,)),
            dma((7,)),
            dma((2, REST)),
            dma((2, REST)),
        ],
        compiler_params=pltpu.CompilerParams(
            collective_id=0, has_side_effects=True, vmem_limit_bytes=32 * 1024 * 1024
        ),
    )(*inputs)


def solution(mesh):
    in_specs = (P("task", None, "shard", None), P("task", None, "shard", None), P("task", None, None))
    return jax.shard_map(on_device, mesh=mesh, in_specs=in_specs, out_specs=P(None, "shard", "task"), check_vma=False)
```

```python
import functools

import jax
import jax.numpy as jnp
from jax import lax
from jax.experimental import pallas as pl
from jax.experimental.pallas import tpu as pltpu
from jax.sharding import PartitionSpec as P

EXPERTS = 8
ROWS = 64
FF = 16384
LAYERS = 4
TASKS = 4
SHARDS = 32
GROUP = 4
HERE = 16
HALF = 2048
LANES = 128
PARTS = HALF // LANES
RAW = 1
REST = LAYERS - RAW

MESH = pl.DeviceIdType.MESH
F32 = jnp.float32
BF16 = jnp.bfloat16


def kernel(
    delta, score, limit_in, out,
    limit, dbuf, sbuf, masked, sums, pair_in, chip_in, half, half_in, prob, inv_own, prob_in, inv, acc, raw_in,
    far, far_in, joint, joint_in, tot, tot_z, tot2, tot_x, grand,
    sem_load, sem_sent, sem_got, sem_f, sem_j,
):
    s, t = lax.axis_index("shard"), lax.axis_index("task")
    expert = lax.div(s, GROUP)
    member = lax.rem(s, GROUP)
    core = lax.rem(s, 2)
    first = expert * GROUP
    late = lax.rem(expert, 2)
    hub = (expert - late) * GROUP
    other = hub + (1 - late) * GROUP

    def at_task(d):
        return (s, lax.rem(t + d, TASKS))

    def at_x(d):
        return (lax.rem(s + 2 * GROUP * d, SHARDS), t)

    def block_of(owner):
        return pl.ds(pl.multiple_of(owner * 2 * HALF, 2 * HALF), 2 * HALF)

    def at_group(d):
        return (first + lax.rem(member + d, GROUP), t)

    def send(src, dst, kind, to, got=None):
        copy = pltpu.make_async_remote_copy(
            src_ref=src, dst_ref=dst, send_sem=sem_sent.at[kind], recv_sem=sem_got.at[kind] if got is None else got,
            device_id=to, device_id_type=MESH,
        )
        copy.start()
        return copy

    def wait(ref, sem):
        pltpu.make_async_copy(ref, ref, sem).wait()

    def shares(ref):
        return {0: ref.at[pl.ds(0, 1)], 1: ref.at[:, pl.ds(0, 2)], 2: ref.at[pl.ds(0, 2)], 4: ref}[RAW]

    PAIR, CHIP, WHOLE, TOTAL, TOTAL_X, GRAND, PROB_Y, ENTRY, FAR, JOINT = range(10)

    barrier = pltpu.get_barrier_semaphore()

    def greet(to):
        pl.semaphore_signal(barrier, inc=1, device_id=to, device_id_type=MESH)

    for d in (1, 2, 3):
        greet(at_task(d))
        greet(at_group(d))

    @pl.when(late == 0)
    def _():
        for d in (1, 2, 3):
            greet(at_x(d))
        for m in range(GROUP):
            greet((other + m, t))

    up, down, far_owner = lax.rem(t + 1, TASKS), lax.rem(t + 3, TASKS), lax.rem(t + 2, TASKS)
    pieces = [(limit_in, limit)]
    for owner in (up, down):
        pieces.append((delta.at[0, 0, :, block_of(owner)], dbuf.at[0, :, block_of(owner)]))
        pieces.append((score.at[0, 0, :, block_of(owner)], sbuf.at[0, :, block_of(owner)]))
    for owner in (far_owner, t):
        pieces.append((delta.at[0, 0, :, block_of(owner)], dbuf.at[0, :, block_of(owner)]))
    rest_l = pl.ds(1, LAYERS - 1)
    pieces.append((delta.at[0, rest_l], dbuf.at[rest_l]))
    for owner in (far_owner, t):
        pieces.append((score.at[0, 0, :, block_of(owner)], sbuf.at[0, :, block_of(owner)]))
    pieces.append((score.at[0, rest_l], sbuf.at[rest_l]))
    loads = [pltpu.make_async_copy(src, dst, sem_load.at[i]) for i, (src, dst) in enumerate(pieces)]
    for load in loads:
        load.start()

    row = lax.broadcasted_iota(jnp.int32, (8, LANES), 0)
    bits = [lax.rem(lax.div(row, 2**k), 2) == 0 for k in range(3)]

    def sum_layer(l):
        def body(i, carry):
            b, h = lax.div(i, 2), lax.rem(i, 2)
            for j0 in range(0, PARTS, 8):
                parts = []
                for j in range(j0, j0 + 8):
                    cols = pl.ds(pl.multiple_of(i * HALF + j * LANES, LANES), LANES)
                    change = jnp.abs(dbuf[l, :, cols].astype(F32))
                    parts.append(change[:8] + change[8:])
                for k, even in enumerate(bits):
                    parts = [
                        jnp.where(even, a, b_) + pltpu.roll(jnp.where(even, b_, a), 2**k, 0)
                        for a, b_ in zip(parts[::2], parts[1::2])
                    ]
                sums[h, b, l, j0 : j0 + 8, :] = parts[0]
            return carry

        lax.fori_loop(0, 2 * TASKS, body, 0)

    def mask_half(l, i):
        b, h = lax.div(i, 2), lax.rem(i, 2)
        own_limit = limit[0, l, expert]
        for j in range(PARTS):
            cols = pl.ds(pl.multiple_of(i * HALF + j * LANES, LANES), LANES)
            keep = sbuf[l, :, cols] < own_limit
            masked[b, l, h, :, j * LANES : (j + 1) * LANES] = jnp.where(
                keep, dbuf[l, :, cols].astype(F32), F32(0.0)
            ).astype(BF16)

    def mask_block(l, owner):
        def body(i, carry):
            mask_half(l, 2 * owner + i)
            return carry

        lax.fori_loop(0, 2, body, 0)

    def mask_layer(l):
        def body(i, carry):
            mask_half(l, i)
            return carry

        lax.fori_loop(0, 2 * TASKS, body, 0)

    flight = []

    def send_raw(l, ds=(1, 3, 2)):
        for d in ds:
            if d == 2 and l >= RAW:
                continue
            owner = lax.rem(t + d, TASKS)
            if l < RAW:
                flight.append(send(masked.at[owner, l], raw_in.at[d - 1, l], ENTRY, at_task(d)))
            else:
                h = 1 if d == 1 else 0
                flight.append(send(masked.at[owner, l, h], raw_in.at[d - 1, l, h], ENTRY, at_task(d)))

    with jax.named_scope("load"):
        for load in loads[:3]:
            load.wait()
    with jax.named_scope("mask0"):
        mask_block(0, up)
    with jax.named_scope("bar"):
        pl.semaphore_wait(barrier, 9 + late)
    send_raw(0, (1,))
    with jax.named_scope("mask1"):
        for load in loads[3:5]:
            load.wait()
        mask_block(0, down)
    send_raw(0, (3,))
    with jax.named_scope("sums"):
        for load in loads[5:8]:
            load.wait()
        for l in range(LAYERS):
            sum_layer(l)

    send(sums.at[1 - core], pair_in, PAIR, at_group(1 - 2 * core + GROUP))

    for l in range(LAYERS):
        whole = sums[0, 0, l] + sums[1, 0, l]
        for b in range(1, TASKS):
            whole = whole + sums[0, b, l] + sums[1, b, l]
        tot[l : l + 1, :] = jnp.sum(whole, axis=0, keepdims=True)
    tot[LAYERS:, :] = jnp.zeros((8 - LAYERS, LANES), F32)

    @pl.when(late == 0)
    def _():
        for d in range(1, GROUP):
            send(tot, tot_z.at[d - 1], TOTAL, at_group(d))

    @pl.when(late == 1)
    def _():
        for m in range(GROUP):
            send(tot, tot_z.at[GROUP - 1 + member], TOTAL, (other + m, t))

    with jax.named_scope("masks"):
        for load, owner in ((loads[8], far_owner), (loads[9], t)):
            load.wait()
            mask_block(0, owner)
        send_raw(0, (2,))
        loads[10].wait()
        for l in range(1, LAYERS):
            mask_layer(l)
            send_raw(l)

    with jax.named_scope("waitpair"):
        wait(pair_in, sem_got.at[PAIR])
    sums[core] = sums[core] + pair_in[...]
    send(sums.at[core], chip_in, CHIP, at_group(2))

    with jax.named_scope("totals1"):

        @pl.when(late == 0)
        def _():
            wait(tot_z, sem_got.at[TOTAL])
            whole = tot[...]
            for d in range(2 * GROUP - 1):
                whole = whole + tot_z[d]
            tot2[...] = whole
            for d in (1, 2, 3):
                send(tot2, tot_x.at[d - 1], TOTAL_X, at_x(d))

    with jax.named_scope("waitchip"):
        wait(chip_in, sem_got.at[CHIP])
    half[...] = sums[core] + chip_in[...]
    send(half, half_in, WHOLE, at_group(1 - 2 * core + GROUP))
    with jax.named_scope("totals2"):

        @pl.when(late == 0)
        def _():
            wait(tot_x, sem_got.at[TOTAL_X])
            grand[...] = tot2[...] + tot_x[0] + tot_x[1] + tot_x[2]
            send(grand, grand, GRAND, (other + member, t))

        @pl.when(late == 1)
        def _():
            wait(grand, sem_got.at[GRAND])

    grand_mean = jnp.sum(grand[...], axis=1, keepdims=True) / F32(EXPERTS * ROWS * FF)
    with jax.named_scope("waitwhole"):
        wait(half_in, sem_got.at[WHOLE])

    def make_prob(b, l):
        mean_l = jnp.broadcast_to(grand_mean[l : l + 1, :], (PARTS, LANES))
        mine, theirs = half[b, l], half_in[b, l]
        for h in range(2):
            column = jnp.where(core == h, mine, theirs) / F32(ROWS)
            rounded = (0.2 + 0.7 * column / (column + mean_l)).astype(BF16)
            prob[b, l, h] = rounded
            inv_own[b, l, h] = 1.0 / rounded.astype(F32)

    def rescaled(block, tile, j):
        return block[:, j * LANES : (j + 1) * LANES].astype(F32) * tile[j : j + 1, :]

    with jax.named_scope("far"):
        for l in range(RAW, LAYERS):
            make_prob(far_owner, l)
            for h in range(2):
                tile = inv_own[far_owner, l, h]
                for j in range(PARTS):
                    far[h, l - RAW, :, j * LANES : (j + 1) * LANES] = rescaled(
                        masked.at[far_owner, l, h], tile, j
                    ).astype(BF16)
                flight.append(
                    send(far.at[h, l - RAW], far_in.at[h, l - RAW], FAR, at_task(3 if h else 1), sem_f.at[h, l - RAW])
                )
    with jax.named_scope("prob"):
        for l in range(RAW):
            make_prob(far_owner, l)
        for owner in (up, down, t):
            for l in range(LAYERS):
                make_prob(owner, l)
    for d in (1, 3):
        owner, h = lax.rem(t + d, TASKS), 1 if d == 1 else 0
        if RAW < LAYERS:
            rest = pl.ds(RAW, LAYERS - RAW)
            send(prob.at[owner, rest, h], prob_in.at[d - 1, rest, h], PROB_Y, at_task(d))
    for d in (1, 3, 2) if RAW else ():
        some = pl.ds(0, RAW)
        send(prob.at[lax.rem(t + d, TASKS), some], prob_in.at[d - 1, some], PROB_Y, at_task(d))

    with jax.named_scope("own"):
        for l in range(LAYERS):
            for h in range(2):
                tile = inv_own[t, l, h]
                for j in range(PARTS):
                    acc[l, h, :, j * LANES : (j + 1) * LANES] = rescaled(masked.at[t, l, h], tile, j)

    for l in range(RAW, LAYERS):
        for h in range(2):
            with jax.named_scope(f"waitfar#l={l}#h={h}"):
                wait(far_in.at[h, l - RAW], sem_f.at[h, l - RAW])
            owner = lax.rem(t + (3 if h else 1), TASKS)
            tile = inv_own[owner, l, h]
            for j in range(PARTS):
                cols = slice(j * LANES, (j + 1) * LANES)
                joint[h, l - RAW, :, cols] = (
                    rescaled(masked.at[owner, l, h], tile, j) + far_in[h, l - RAW, :, cols].astype(F32)
                ).astype(BF16)
            send(joint.at[h, l - RAW], joint_in.at[h, l - RAW], JOINT, at_task(3 if h else 1), sem_j.at[h, l - RAW])

    with jax.named_scope("waitpy"):
        wait(shares(prob_in), sem_got.at[PROB_Y])
    for d in (1, 2, 3):
        for l in range(LAYERS):
            for h in range(2):
                if l < RAW or (d, h) in ((1, 1), (3, 0)):
                    inv[d - 1, l, h] = 1.0 / prob_in[d - 1, l, h].astype(F32)
    with jax.named_scope("waitraw"):
        wait(shares(raw_in), sem_got.at[ENTRY])
    with jax.named_scope("raw"):
        for l in range(LAYERS):
            for h in range(2):
                sources = (1, 2, 3) if l < RAW else (1,) if h else (3,)
                tiles = {d: inv[d - 1, l, h] for d in sources}
                for j in range(PARTS):
                    cols = slice(j * LANES, (j + 1) * LANES)
                    here = acc[l, h, :, cols]
                    for d in sources:
                        here = here + rescaled(raw_in.at[d - 1, l, h], tiles[d], j)
                    if l < RAW:
                        out[l, :, h * HALF + j * LANES : h * HALF + (j + 1) * LANES] = here.astype(BF16)
                    else:
                        acc[l, h, :, cols] = here
    for l in range(RAW, LAYERS):
        for h in range(2):
            with jax.named_scope(f"waitjoint#l={l}#h={h}"):
                wait(joint_in.at[h, l - RAW], sem_j.at[h, l - RAW])
            for j in range(PARTS):
                cols = slice(j * LANES, (j + 1) * LANES)
                out[l, :, h * HALF + j * LANES : h * HALF + (j + 1) * LANES] = (
                    acc[l, h, :, cols] + joint_in[h, l - RAW, :, cols].astype(F32)
                ).astype(BF16)

    with jax.named_scope("waitsend"):

        @pl.when(late == 0)
        def _():
            wait(tot_z.at[pl.ds(0, GROUP - 1)], sem_sent.at[TOTAL])
            wait(tot_x, sem_sent.at[TOTAL_X])
            wait(grand, sem_sent.at[GRAND])

        @pl.when(late == 1)
        def _():
            wait(tot_z.at[pl.ds(0, GROUP)], sem_sent.at[TOTAL])

        wait(pair_in, sem_sent.at[PAIR])
        wait(chip_in, sem_sent.at[CHIP])
        wait(half, sem_sent.at[WHOLE])
        wait(shares(prob_in), sem_sent.at[PROB_Y])
        wait(shares(raw_in), sem_sent.at[ENTRY])
        if RAW < LAYERS:
            wait(far, sem_sent.at[FAR])
            wait(joint, sem_sent.at[JOINT])


def on_device(task_deltas, rank_scores, keep_limits):
    dma = pltpu.SemaphoreType.DMA
    inputs = (pltpu.with_memory_space_constraint(x, pltpu.HBM) for x in (task_deltas, rank_scores, keep_limits))
    return pl.pallas_call(
        kernel,
        out_shape=jax.ShapeDtypeStruct((LAYERS, HERE, 2 * HALF), BF16),
        in_specs=[pl.BlockSpec(memory_space=pl.ANY)] * 3,
        out_specs=pl.BlockSpec(memory_space=pltpu.VMEM),
        scratch_shapes=[
            pltpu.SMEM((1, LAYERS, EXPERTS), jnp.int32),
            pltpu.VMEM((LAYERS, HERE, FF), BF16),
            pltpu.VMEM((LAYERS, HERE, FF), jnp.int32),
            pltpu.VMEM((TASKS, LAYERS, 2, HERE, HALF), BF16),
            pltpu.VMEM((2, TASKS, LAYERS, PARTS, LANES), F32),
            *[pltpu.VMEM((TASKS, LAYERS, PARTS, LANES), F32)] * 4,
            pltpu.VMEM((TASKS, LAYERS, 2, PARTS, LANES), BF16),
            pltpu.VMEM((TASKS, LAYERS, 2, PARTS, LANES), F32),
            pltpu.VMEM((3, LAYERS, 2, PARTS, LANES), BF16),
            pltpu.VMEM((3, LAYERS, 2, PARTS, LANES), F32),
            pltpu.VMEM((LAYERS, 2, HERE, HALF), F32),
            pltpu.VMEM((3, LAYERS, 2, HERE, HALF), BF16),
            *[pltpu.VMEM((2, REST, HERE, HALF), BF16)] * 4,
            pltpu.VMEM((8, LANES), F32),
            pltpu.VMEM((2 * GROUP - 1, 8, LANES), F32),
            pltpu.VMEM((8, LANES), F32),
            pltpu.VMEM((3, 8, LANES), F32),
            pltpu.VMEM((8, LANES), F32),
            dma((11,)),
            dma((10,)),
            dma((8,)),
            dma((2, REST)),
            dma((2, REST)),
        ],
        compiler_params=pltpu.CompilerParams(
            collective_id=0, has_side_effects=True, vmem_limit_bytes=32 * 1024 * 1024
        ),
    )(*inputs)


def solution(mesh):
    in_specs = (P("task", None, "shard", None), P("task", None, "shard", None), P("task", None, None))
    return jax.shard_map(on_device, mesh=mesh, in_specs=in_specs, out_specs=P(None, "shard", "task"), check_vma=False)
```

```python
import functools

import jax
import jax.numpy as jnp
from jax import lax
from jax.experimental import pallas as pl
from jax.experimental.pallas import tpu as pltpu
from jax.sharding import PartitionSpec as P

EXPERTS = 8
ROWS = 64
FF = 16384
LAYERS = 4
TASKS = 4
SHARDS = 32
GROUP = 4
HERE = 16
HALF = 2048
LANES = 128
PARTS = HALF // LANES
RAW = 1
REST = LAYERS - RAW

MESH = pl.DeviceIdType.MESH
F32 = jnp.float32
BF16 = jnp.bfloat16


def kernel(
    delta, score, limit_in, out,
    limit, dbuf, sbuf, masked, sums, pair_in, chip_out, chip_in, half, half_in, prob, inv_own, prob_in, inv, acc, raw_in,
    far, far_in, joint, joint_in, tot, tot_z, tot2, tot_x, grand,
    sem_load, sem_sent, sem_got, sem_f, sem_j, sem_near,
):
    s, t = lax.axis_index("shard"), lax.axis_index("task")
    expert = lax.div(s, GROUP)
    member = lax.rem(s, GROUP)
    core = lax.rem(s, 2)
    first = expert * GROUP
    late = lax.rem(expert, 2)
    other = (expert + 1 - 2 * late) * GROUP
    hub = jnp.logical_and(late == 0, core == 1)

    def at_task(d):
        return (s, lax.rem(t + d, TASKS))

    def at_x(d):
        return (lax.rem(s + 2 * GROUP * d, SHARDS), t)

    def at_other(m):
        return (other + m, t)

    def block_of(owner):
        return pl.ds(pl.multiple_of(owner * 2 * HALF, 2 * HALF), 2 * HALF)

    def at_group(d):
        return (first + lax.rem(member + d, GROUP), t)

    def send(src, dst, kind, to, got=None, done=False):
        copy = pltpu.make_async_remote_copy(
            src_ref=src, dst_ref=dst, send_sem=sem_sent.at[kind], recv_sem=sem_got.at[kind] if got is None else got,
            device_id=to, device_id_type=MESH,
        )
        copy.start()
        return None if done else copy

    def wait(ref, sem):
        pltpu.make_async_copy(ref, ref, sem).wait()

    def shares(ref):
        return {0: ref.at[pl.ds(0, 1)], 1: ref.at[:, pl.ds(0, 2)], 2: ref.at[pl.ds(0, 2)], 4: ref}[RAW]

    PAIR, CHIP, WHOLE, TOTAL, TOTAL_X, GRAND, PROB_Y, ENTRY, FAR, JOINT = range(10)

    barrier = pltpu.get_barrier_semaphore()

    def greet(to):
        pl.semaphore_signal(barrier, inc=1, device_id=to, device_id_type=MESH)

    wide = t < 2
    at_x0 = lax.div(s, 2 * GROUP)
    for d in (1, 2, 3):
        greet(at_task(d))
        pl.when(jnp.logical_or(wide, member + d < GROUP))(functools.partial(greet, at_group(d)))

    @pl.when(hub)
    def _():
        for d in (1, 2, 3):
            pl.when(jnp.logical_or(wide, at_x0 + d < SHARDS // (2 * GROUP)))(functools.partial(greet, at_x(d)))
        for m in range(GROUP):
            greet(at_other(m))

    up, down, far_owner = lax.rem(t + 1, TASKS), lax.rem(t + 3, TASKS), lax.rem(t + 2, TASKS)
    pieces = [(limit_in, limit)]
    for owner in (up, down):
        pieces.append((delta.at[0, 0, :, block_of(owner)], dbuf.at[0, :, block_of(owner)]))
        pieces.append((score.at[0, 0, :, block_of(owner)], sbuf.at[0, :, block_of(owner)]))
    for owner in (far_owner, t):
        pieces.append((delta.at[0, 0, :, block_of(owner)], dbuf.at[0, :, block_of(owner)]))
    for l in range(1, LAYERS):
        pieces.append((delta.at[0, l], dbuf.at[l]))
    for owner in (far_owner, t):
        pieces.append((score.at[0, 0, :, block_of(owner)], sbuf.at[0, :, block_of(owner)]))
    for l in range(1, LAYERS):
        pieces.append((score.at[0, l], sbuf.at[l]))
    loads = [pltpu.make_async_copy(src, dst, sem_load.at[i]) for i, (src, dst) in enumerate(pieces)]
    for load in loads:
        load.start()

    row = lax.broadcasted_iota(jnp.int32, (8, LANES), 0)
    bits = [lax.rem(lax.div(row, 2**k), 2) == 0 for k in range(3)]

    def sum_layer(l):
        def body(i, carry):
            b, h = lax.div(i, 2), lax.rem(i, 2)
            for j0 in range(0, PARTS, 8):
                parts = []
                for j in range(j0, j0 + 8):
                    cols = pl.ds(pl.multiple_of(i * HALF + j * LANES, LANES), LANES)
                    change = jnp.abs(dbuf[l, :, cols].astype(F32))
                    parts.append(change[:8] + change[8:])
                for k, even in enumerate(bits):
                    parts = [
                        jnp.where(even, a, b_) + pltpu.roll(jnp.where(even, b_, a), 2**k, 0)
                        for a, b_ in zip(parts[::2], parts[1::2])
                    ]
                sums[h, b, l, j0 : j0 + 8, :] = parts[0]
            return carry

        lax.fori_loop(0, 2 * TASKS, body, 0)

    def mask_half(l, i):
        b, h = lax.div(i, 2), lax.rem(i, 2)
        own_limit = limit[0, l, expert]
        for j in range(PARTS):
            cols = pl.ds(pl.multiple_of(i * HALF + j * LANES, LANES), LANES)
            keep = sbuf[l, :, cols] < own_limit
            masked[b, l, h, :, j * LANES : (j + 1) * LANES] = jnp.where(
                keep, dbuf[l, :, cols].astype(F32), F32(0.0)
            ).astype(BF16)

    def mask_block(l, owner):
        def body(i, carry):
            mask_half(l, 2 * owner + i)
            return carry

        lax.fori_loop(0, 2, body, 0)

    def mask_layer(l):
        def body(i, carry):
            mask_half(l, i)
            return carry

        lax.fori_loop(0, 2 * TASKS, body, 0)

    flight = []

    def send_raw(l, ds=(1, 3, 2)):
        for d in ds:
            if d == 2 and l >= RAW:
                continue
            owner = lax.rem(t + d, TASKS)
            if l < RAW:
                flight.append(send(masked.at[owner, l], raw_in.at[d - 1, l], ENTRY, at_task(d)))
            else:
                h = 1 if d == 1 else 0
                flight.append(send(masked.at[owner, l, h], raw_in.at[d - 1, l, h], ENTRY, at_task(d)))

    with jax.named_scope("load"):
        for load in loads[:3]:
            load.wait()
    with jax.named_scope("mask0"):
        mask_block(0, up)

    def all_sums():
        for l in range(LAYERS):
            for load in loads[5:7] if l == 0 else loads[6 + l : 7 + l]:
                load.wait()
            sum_layer(l)

    def mask_down():
        for load in loads[3:5]:
            load.wait()
        mask_block(0, down)

    with jax.named_scope("sums0"):

        @pl.when(t < 2)
        def _():
            mask_down()
            all_sums()

    with jax.named_scope("bar"):
        met = jnp.where(wide, GROUP - 1, member) + 2 * late + jnp.where(hub, jnp.where(wide, GROUP - 1, at_x0), 0)
        pl.semaphore_wait(barrier, TASKS - 1 + met)
    send_raw(0, (1,))

    @pl.when(jnp.logical_not(wide))
    def _():
        for d in (1, 2, 3):
            for back, peer in (
                (member - d >= 0, at_group(4 - d)),
                (jnp.logical_and(hub, at_x0 - d >= 0), at_x(4 - d)),
            ):

                @pl.when(back)
                def _():
                    pl.semaphore_signal(sem_near, inc=1, device_id=peer, device_id_type=MESH)

    with jax.named_scope("mask1"):
        pl.when(t >= 2)(mask_down)
    send_raw(0, (3,))
    with jax.named_scope("sums1"):
        pl.when(t >= 2)(all_sums)

    for l in range(LAYERS):
        whole = sums[0, 0, l] + sums[1, 0, l]
        for b in range(1, TASKS):
            whole = whole + sums[0, b, l] + sums[1, b, l]
        tot[l : l + 1, :] = jnp.sum(whole, axis=0, keepdims=True)
    tot[LAYERS:, :] = jnp.zeros((8 - LAYERS, LANES), F32)

    @pl.when(late == 1)
    def _():
        for m in (1, 3):
            send(tot, tot_z.at[GROUP - 1 + member], TOTAL, at_other(m))

    with jax.named_scope("near"):

        to_come = GROUP - 1 - member + jnp.where(hub, GROUP - 1 - at_x0, 0)

        @pl.when(jnp.logical_and(jnp.logical_not(wide), to_come > 0))
        def _():
            pl.semaphore_wait(sem_near, to_come)

    send(sums.at[1 - core], pair_in, PAIR, at_group(1 - 2 * core + GROUP))

    @pl.when(late == 0)
    def _():
        for d in range(1, GROUP):
            pl.when(lax.rem(member + d, 2) == 1)(
                functools.partial(send, tot, tot_z.at[d - 1], TOTAL, at_group(d), done=True)
            )

    with jax.named_scope("masks"):
        for load, owner in ((loads[10], far_owner), (loads[11], t)):
            load.wait()
            mask_block(0, owner)
        send_raw(0, (2,))
        for l in range(1, LAYERS):
            loads[11 + l].wait()
            mask_layer(l)
            send_raw(l)

    with jax.named_scope("waitpair"):
        wait(pair_in, sem_got.at[PAIR])
    half[...] = sums[core] + pair_in[...]
    chip_out[...] = half[...]
    send(chip_out, chip_in, CHIP, at_group(2))

    with jax.named_scope("totals1"):

        @pl.when(hub)
        def _():
            wait(tot_z, sem_got.at[TOTAL])
            whole = tot[...]
            for d in range(2 * GROUP - 1):
                whole = whole + tot_z[d]
            tot2[...] = whole
            for d in (1, 2, 3):
                send(tot2, tot_x.at[d - 1], TOTAL_X, at_x(d))

    with jax.named_scope("waitchip"):
        wait(chip_in, sem_got.at[CHIP])
    half[...] = chip_out[...] + chip_in[...]
    send(half, half_in, WHOLE, at_group(1 - 2 * core + GROUP))
    with jax.named_scope("totals2"):

        @pl.when(hub)
        def _():
            wait(tot_x, sem_got.at[TOTAL_X])
            grand[...] = tot2[...] + tot_x[0] + tot_x[1] + tot_x[2]
            send(grand, grand, GRAND, at_other(GROUP - 1 - member))
            send(grand, grand, GRAND, at_other(GROUP - member))
            send(grand, grand, GRAND, at_group(GROUP - 1))

        @pl.when(jnp.logical_not(hub))
        def _():
            wait(grand, sem_got.at[GRAND])

    grand_mean = jnp.sum(grand[...], axis=1, keepdims=True) / F32(EXPERTS * ROWS * FF)
    with jax.named_scope("waitwhole"):
        wait(half_in, sem_got.at[WHOLE])

    def make_prob(b, l):
        mean_l = jnp.broadcast_to(grand_mean[l : l + 1, :], (PARTS, LANES))
        mine, theirs = half[b, l], half_in[b, l]
        for h in range(2):
            column = jnp.where(core == h, mine, theirs) / F32(ROWS)
            rounded = (0.2 + 0.7 * column / (column + mean_l)).astype(BF16)
            prob[b, l, h] = rounded
            inv_own[b, l, h] = 1.0 / rounded.astype(F32)

    def rescaled(block, tile, j):
        return block[:, j * LANES : (j + 1) * LANES].astype(F32) * tile[j : j + 1, :]

    with jax.named_scope("far"):
        for l in range(RAW, LAYERS):
            make_prob(far_owner, l)
            for h in range(2):
                tile = inv_own[far_owner, l, h]
                for j in range(PARTS):
                    far[h, l - RAW, :, j * LANES : (j + 1) * LANES] = rescaled(
                        masked.at[far_owner, l, h], tile, j
                    ).astype(BF16)
                flight.append(
                    send(far.at[h, l - RAW], far_in.at[h, l - RAW], FAR, at_task(3 if h else 1), sem_f.at[h, l - RAW])
                )
    with jax.named_scope("prob"):
        for l in range(RAW):
            make_prob(far_owner, l)
        for owner in (up, down, t):
            for l in range(LAYERS):
                make_prob(owner, l)
    for d in (1, 3):
        owner, h = lax.rem(t + d, TASKS), 1 if d == 1 else 0
        if RAW < LAYERS:
            rest = pl.ds(RAW, LAYERS - RAW)
            send(prob.at[owner, rest, h], prob_in.at[d - 1, rest, h], PROB_Y, at_task(d))
    for d in (1, 3, 2) if RAW else ():
        some = pl.ds(0, RAW)
        send(prob.at[lax.rem(t + d, TASKS), some], prob_in.at[d - 1, some], PROB_Y, at_task(d))

    with jax.named_scope("own"):
        for l in range(LAYERS):
            for h in range(2):
                tile = inv_own[t, l, h]
                for j in range(PARTS):
                    acc[l, h, :, j * LANES : (j + 1) * LANES] = rescaled(masked.at[t, l, h], tile, j)

    for l in range(RAW, LAYERS):
        for h in range(2):
            with jax.named_scope(f"waitfar#l={l}#h={h}"):
                wait(far_in.at[h, l - RAW], sem_f.at[h, l - RAW])
            owner = lax.rem(t + (3 if h else 1), TASKS)
            tile = inv_own[owner, l, h]
            for j in range(PARTS):
                cols = slice(j * LANES, (j + 1) * LANES)
                joint[h, l - RAW, :, cols] = (
                    rescaled(masked.at[owner, l, h], tile, j) + far_in[h, l - RAW, :, cols].astype(F32)
                ).astype(BF16)
            send(joint.at[h, l - RAW], joint_in.at[h, l - RAW], JOINT, at_task(3 if h else 1), sem_j.at[h, l - RAW])

    with jax.named_scope("waitpy"):
        wait(shares(prob_in), sem_got.at[PROB_Y])
    for d in (1, 2, 3):
        for l in range(LAYERS):
            for h in range(2):
                if l < RAW or (d, h) in ((1, 1), (3, 0)):
                    inv[d - 1, l, h] = 1.0 / prob_in[d - 1, l, h].astype(F32)
    with jax.named_scope("waitraw"):
        wait(shares(raw_in), sem_got.at[ENTRY])
    with jax.named_scope("raw"):
        for l in range(LAYERS):
            for h in range(2):
                sources = (1, 2, 3) if l < RAW else (1,) if h else (3,)
                tiles = {d: inv[d - 1, l, h] for d in sources}
                for j in range(PARTS):
                    cols = slice(j * LANES, (j + 1) * LANES)
                    here = acc[l, h, :, cols]
                    for d in sources:
                        here = here + rescaled(raw_in.at[d - 1, l, h], tiles[d], j)
                    if l < RAW:
                        out[l, :, h * HALF + j * LANES : h * HALF + (j + 1) * LANES] = here.astype(BF16)
                    else:
                        acc[l, h, :, cols] = here
    for l in range(RAW, LAYERS):
        for h in range(2):
            with jax.named_scope(f"waitjoint#l={l}#h={h}"):
                wait(joint_in.at[h, l - RAW], sem_j.at[h, l - RAW])
            for j in range(PARTS):
                cols = slice(j * LANES, (j + 1) * LANES)
                out[l, :, h * HALF + j * LANES : h * HALF + (j + 1) * LANES] = (
                    acc[l, h, :, cols] + joint_in[h, l - RAW, :, cols].astype(F32)
                ).astype(BF16)

    with jax.named_scope("waitsend"):
        @pl.when(hub)
        def _():
            wait(tot_z.at[0], sem_sent.at[TOTAL])
            wait(tot_x, sem_sent.at[TOTAL_X])
            wait(tot_x, sem_sent.at[GRAND])

        @pl.when(jnp.logical_not(hub))
        def _():
            wait(tot_z.at[pl.ds(0, 2)], sem_sent.at[TOTAL])

        wait(pair_in, sem_sent.at[PAIR])
        wait(chip_in, sem_sent.at[CHIP])
        wait(half, sem_sent.at[WHOLE])
        wait(shares(prob_in), sem_sent.at[PROB_Y])
        wait(shares(raw_in), sem_sent.at[ENTRY])
        if RAW < LAYERS:
            wait(far, sem_sent.at[FAR])
            wait(joint, sem_sent.at[JOINT])


def on_device(task_deltas, rank_scores, keep_limits):
    dma = pltpu.SemaphoreType.DMA
    inputs = (pltpu.with_memory_space_constraint(x, pltpu.HBM) for x in (task_deltas, rank_scores, keep_limits))
    return pl.pallas_call(
        kernel,
        out_shape=jax.ShapeDtypeStruct((LAYERS, HERE, 2 * HALF), BF16),
        in_specs=[pl.BlockSpec(memory_space=pl.ANY)] * 3,
        out_specs=pl.BlockSpec(memory_space=pltpu.VMEM),
        scratch_shapes=[
            pltpu.SMEM((1, LAYERS, EXPERTS), jnp.int32),
            pltpu.VMEM((LAYERS, HERE, FF), BF16),
            pltpu.VMEM((LAYERS, HERE, FF), jnp.int32),
            pltpu.VMEM((TASKS, LAYERS, 2, HERE, HALF), BF16),
            pltpu.VMEM((2, TASKS, LAYERS, PARTS, LANES), F32),
            pltpu.VMEM((TASKS, LAYERS, PARTS, LANES), F32),
            *[pltpu.VMEM((TASKS, LAYERS, PARTS, LANES), F32)] * 4,
            pltpu.VMEM((TASKS, LAYERS, 2, PARTS, LANES), BF16),
            pltpu.VMEM((TASKS, LAYERS, 2, PARTS, LANES), F32),
            pltpu.VMEM((3, LAYERS, 2, PARTS, LANES), BF16),
            pltpu.VMEM((3, LAYERS, 2, PARTS, LANES), F32),
            pltpu.VMEM((LAYERS, 2, HERE, HALF), F32),
            pltpu.VMEM((3, LAYERS, 2, HERE, HALF), BF16),
            *[pltpu.VMEM((2, REST, HERE, HALF), BF16)] * 4,
            pltpu.VMEM((8, LANES), F32),
            pltpu.VMEM((2 * GROUP - 1, 8, LANES), F32),
            pltpu.VMEM((8, LANES), F32),
            pltpu.VMEM((3, 8, LANES), F32),
            pltpu.VMEM((8, LANES), F32),
            dma((15,)),
            dma((10,)),
            dma((8,)),
            dma((2, REST)),
            dma((2, REST)),
            pltpu.SemaphoreType.REGULAR,
        ],
        compiler_params=pltpu.CompilerParams(
            collective_id=0, has_side_effects=True, vmem_limit_bytes=32 * 1024 * 1024
        ),
    )(*inputs)


def solution(mesh):
    in_specs = (P("task", None, "shard", None), P("task", None, "shard", None), P("task", None, None))
    return jax.shard_map(on_device, mesh=mesh, in_specs=in_specs, out_specs=P(None, "shard", "task"), check_vma=False)
```

```python
import functools

import jax
import jax.numpy as jnp
from jax import lax
from jax.experimental import pallas as pl
from jax.experimental.pallas import tpu as pltpu
from jax.sharding import PartitionSpec as P

EXPERTS = 8
ROWS = 64
FF = 16384
LAYERS = 4
TASKS = 4
SHARDS = 32
GROUP = 4
HERE = 16
HALF = 2048
LANES = 128
PARTS = HALF // LANES
HELD = 1

MESH = pl.DeviceIdType.MESH
F32 = jnp.float32
BF16 = jnp.bfloat16


def kernel(
    delta, score, limit_in, out,
    limit, dbuf, sbuf, masked, sums, pair_in, chip_out, chip_in, half, half_in, prob, inv_own, prob_in, far_prob, acc, raw_in,
    far_in, joint, joint_in, tot, tot_z, tot2, tot_x, grand,
    sem_load, sem_sent, sem_got, sem_j, sem_near, sem_line,
):
    s, t = lax.axis_index("shard"), lax.axis_index("task")
    expert = lax.div(s, GROUP)
    member = lax.rem(s, GROUP)
    core = lax.rem(s, 2)
    first = expert * GROUP
    late = lax.rem(expert, 2)
    other = (expert + 1 - 2 * late) * GROUP
    hub = jnp.logical_and(late == 0, core == 1)

    def at_task(d):
        return (s, lax.rem(t + d, TASKS))

    def at_x(d):
        return (lax.rem(s + 2 * GROUP * d, SHARDS), t)

    def at_other(m):
        return (other + m, t)

    def block_of(owner):
        return pl.ds(pl.multiple_of(owner * 2 * HALF, 2 * HALF), 2 * HALF)

    def at_group(d):
        return (first + lax.rem(member + d, GROUP), t)

    def send(src, dst, kind, sent, to, got=None):
        copy = pltpu.make_async_remote_copy(
            src_ref=src, dst_ref=dst, send_sem=sem_sent.at[sent], recv_sem=sem_got.at[kind] if got is None else got,
            device_id=to, device_id_type=MESH,
        )
        copy.start()

    def wait(ref, sem):
        pltpu.make_async_copy(ref, ref, sem).wait()

    PAIR, CHIP, WHOLE, TOTAL, TOTAL_X, GRAND, PROB_F, PROB_Y, NEAR, FAR = range(10)
    COLUMNS, TOTALS, PROBS, ENTRIES = range(4)

    barrier = pltpu.get_barrier_semaphore()

    def greet(to):
        pl.semaphore_signal(barrier, inc=1, device_id=to, device_id_type=MESH)

    wide = t < 2
    at_x0 = lax.div(s, 2 * GROUP)
    greet(at_task(1))
    greet(at_task(3))
    for d in (1, 2, 3):
        pl.when(jnp.logical_or(wide, member + d < GROUP))(functools.partial(greet, at_group(d)))

    @pl.when(hub)
    def _():
        for d in (1, 2, 3):
            pl.when(jnp.logical_or(wide, at_x0 + d < SHARDS // (2 * GROUP)))(functools.partial(greet, at_x(d)))
        for m in range(GROUP):
            greet(at_other(m))

    up, down, far_owner = lax.rem(t + 1, TASKS), lax.rem(t + 3, TASKS), lax.rem(t + 2, TASKS)
    first_d, first_s = delta.at[0, 0], score.at[0, 0]
    pieces = [(limit_in, limit, 0)]
    pieces.append((first_d.at[:, block_of(far_owner)], dbuf.at[0, :, block_of(far_owner)], 1))
    pieces.append((first_s.at[:, block_of(far_owner)], sbuf.at[0, :, block_of(far_owner)], 1))
    for owner in (up, down):
        pieces.append((first_d.at[:, block_of(owner)], dbuf.at[0, :, block_of(owner)], 2))
    pieces.append((first_d.at[:, block_of(t)], dbuf.at[0, :, block_of(t)], 3))
    for l in range(1, LAYERS):
        pieces.append((delta.at[0, l], dbuf.at[l], 3 + l))
    for owner in (up, down):
        pieces.append((first_s.at[:, block_of(owner)], sbuf.at[0, :, block_of(owner)], 7))
    pieces.append((first_s.at[:, block_of(t)], sbuf.at[0, :, block_of(t)], 8))
    pieces.append((score.at[0, pl.ds(1, LAYERS - 1)], sbuf.at[pl.ds(1, LAYERS - 1)], 9))
    loads = [pltpu.make_async_copy(src, dst, sem_load.at[i]) for src, dst, i in pieces]
    for load in loads:
        load.start()

    place = lax.broadcasted_iota(jnp.int32, (PARTS, PARTS * HERE), 1) - HERE * lax.broadcasted_iota(
        jnp.int32, (PARTS, PARTS * HERE), 0
    )
    pick = jnp.where(jnp.logical_and(place >= 0, place < HERE), F32(1.0), F32(0.0)).astype(BF16)

    def sum_layer(l):
        def body(i, carry):
            b, h = lax.div(i, 2), lax.rem(i, 2)
            blocks = [
                jnp.abs(dbuf[l, :, pl.ds(pl.multiple_of(i * HALF + j * LANES, LANES), LANES)]) for j in range(PARTS)
            ]
            sums[h, b, l] = jnp.dot(pick, jnp.concatenate(blocks, axis=0), preferred_element_type=F32)
            return carry

        lax.fori_loop(0, 2 * TASKS, body, 0, unroll=True)

    def mask_half(l, i):
        b, h = lax.div(i, 2), lax.rem(i, 2)
        own_limit = limit[0, l, expert]
        for j in range(PARTS):
            cols = pl.ds(pl.multiple_of(i * HALF + j * LANES, LANES), LANES)
            keep = sbuf[l, :, cols] < own_limit
            masked[b, l, h, :, j * LANES : (j + 1) * LANES] = jnp.where(
                keep, dbuf[l, :, cols].astype(F32), F32(0.0)
            ).astype(BF16)

    def mask_block(l, owner):
        def body(i, carry):
            mask_half(l, 2 * owner + i)
            return carry

        lax.fori_loop(0, 2, body, 0)

    def mask_layer(l):
        def body(i, carry):
            mask_half(l, i)
            return carry

        lax.fori_loop(0, 2 * TASKS, body, 0)

    def send_far(l):
        for h in range(2):
            send(masked.at[far_owner, l, h], far_in.at[h, l], FAR, ENTRIES, at_task(3 if h else 1))

    def send_near(l):
        for d, owner, h in ((1, up, 1), (3, down, 0)):
            send(masked.at[owner, l, h], raw_in.at[h, l], NEAR, ENTRIES, at_task(d))

    with jax.named_scope("load"):
        loads[0].wait()
        wait(sbuf.at[0, :, pl.ds(0, 3 * HALF)], sem_load.at[1])
    with jax.named_scope("mask0"):
        mask_block(0, far_owner)

    def all_sums():
        wait(dbuf.at[0, :, pl.ds(0, 4 * HALF)], sem_load.at[2])
        for l in range(LAYERS):
            wait(dbuf.at[l] if l else dbuf.at[0, :, pl.ds(0, 2 * HALF)], sem_load.at[3 + l])
            sum_layer(l)

    def mask_near():
        wait(sbuf.at[0, :, pl.ds(0, 4 * HALF)], sem_load.at[7])
        mask_block(0, up)
        mask_block(0, down)

    with jax.named_scope("sums0"):

        @pl.when(t < 2)
        def _():
            all_sums()
            mask_near()

    with jax.named_scope("bar"):
        met = jnp.where(wide, GROUP - 1, member) + 2 * late + jnp.where(hub, jnp.where(wide, GROUP - 1, at_x0), 0)
        pl.semaphore_wait(barrier, 2 + met)
    send_far(0)

    @pl.when(jnp.logical_not(wide))
    def _():
        for d in (1, 2, 3):
            for back, peer, sem in (
                (member - d >= 0, at_group(4 - d), sem_near),
                (jnp.logical_and(hub, at_x0 - d >= 0), at_x(4 - d), sem_line),
            ):

                @pl.when(back)
                def _():
                    pl.semaphore_signal(sem, inc=1, device_id=peer, device_id_type=MESH)

    with jax.named_scope("sums1"):

        @pl.when(t >= 2)
        def _():
            all_sums()
            mask_near()

    send_near(0)

    for l in range(LAYERS):
        whole = sums[0, 0, l] + sums[1, 0, l]
        for b in range(1, TASKS):
            whole = whole + sums[0, b, l] + sums[1, b, l]
        tot[l : l + 1, :] = jnp.sum(whole, axis=0, keepdims=True)
    tot[LAYERS:, :] = jnp.zeros((8 - LAYERS, LANES), F32)

    @pl.when(late == 1)
    def _():
        for m in (1, 3):
            send(tot, tot_z.at[GROUP - 1 + member], TOTAL, TOTALS, at_other(m))

    with jax.named_scope("near"):

        to_come = GROUP - 1 - member

        @pl.when(jnp.logical_and(jnp.logical_not(wide), to_come > 0))
        def _():
            pl.semaphore_wait(sem_near, to_come)

    send(sums.at[1 - core], pair_in, PAIR, COLUMNS, at_group(1 - 2 * core + GROUP))

    @pl.when(late == 0)
    def _():
        for d in range(1, GROUP):
            pl.when(lax.rem(member + d, 2) == 1)(
                functools.partial(send, tot, tot_z.at[d - 1], TOTAL, TOTALS, at_group(d))
            )

    with jax.named_scope("masks"):
        wait(sbuf.at[0, :, pl.ds(0, 2 * HALF)], sem_load.at[8])
        mask_block(0, t)
        wait(sbuf.at[pl.ds(1, LAYERS - 1)], sem_load.at[9])
        for l in range(1, LAYERS):
            mask_layer(l)
            send_far(l)
        for l in range(1, LAYERS - HELD):
            send_near(l)

    with jax.named_scope("waitpair"):
        wait(pair_in, sem_got.at[PAIR])
    half[...] = sums[core] + pair_in[...]
    chip_out[...] = half[...]
    send(chip_out, chip_in, CHIP, COLUMNS, at_group(2))

    with jax.named_scope("totals1"):

        @pl.when(hub)
        def _():
            wait(tot_z, sem_got.at[TOTAL])
            whole = tot[...]
            for d in range(2 * GROUP - 1):
                whole = whole + tot_z[d]
            tot2[...] = whole
            to_come_x = GROUP - 1 - at_x0

            @pl.when(jnp.logical_and(jnp.logical_not(wide), to_come_x > 0))
            def _():
                pl.semaphore_wait(sem_line, to_come_x)

            for d in (1, 2, 3):
                send(tot2, tot_x.at[d - 1], TOTAL_X, TOTALS, at_x(d))

    with jax.named_scope("waitchip"):
        wait(chip_in, sem_got.at[CHIP])
    half[...] = chip_out[...] + chip_in[...]
    send(half, half_in, WHOLE, COLUMNS, at_group(1 - 2 * core + GROUP))
    with jax.named_scope("totals2"):

        @pl.when(hub)
        def _():
            wait(tot_x, sem_got.at[TOTAL_X])
            grand[...] = tot2[...] + tot_x[0] + tot_x[1] + tot_x[2]
            send(grand, grand, GRAND, TOTALS, at_other(GROUP - 1 - member))
            send(grand, grand, GRAND, TOTALS, at_other(GROUP - member))
            send(grand, grand, GRAND, TOTALS, at_group(GROUP - 1))

        @pl.when(jnp.logical_not(hub))
        def _():
            wait(grand, sem_got.at[GRAND])

    grand_mean = jnp.sum(grand[...], axis=1, keepdims=True) / F32(EXPERTS * ROWS * FF)
    with jax.named_scope("waitwhole"):
        wait(half_in, sem_got.at[WHOLE])

    def make_prob(b, l):
        mean_l = jnp.broadcast_to(grand_mean[l : l + 1, :], (PARTS, LANES))
        mine, theirs = half[b, l], half_in[b, l]
        for h in range(2):
            column = jnp.where(core == h, mine, theirs) / F32(ROWS)
            rounded = (0.2 + 0.7 * column / (column + mean_l)).astype(BF16)
            prob[b, l, h] = rounded
            inv_own[b, l, h] = 1.0 / rounded.astype(F32)

    def rescaled(block, tile, j):
        return block[:, j * LANES : (j + 1) * LANES].astype(F32) * tile[j : j + 1, :]

    with jax.named_scope("farprob"):
        for l in range(LAYERS):
            make_prob(far_owner, l)
        for h in range(2):
            send(prob.at[far_owner, :, h], far_prob.at[h], PROB_F, PROBS, at_task(3 if h else 1))
    with jax.named_scope("prob"):
        for owner in (up, down, t):
            for l in range(LAYERS):
                make_prob(owner, l)
    for l in range(LAYERS - HELD, LAYERS):
        send_near(l)
    for d, owner, h in ((1, up, 1), (3, down, 0)):
        send(prob.at[owner, :, h], prob_in.at[h], PROB_Y, PROBS, at_task(d))

    with jax.named_scope("own"):
        for l in range(LAYERS):
            for h in range(2):
                tile = inv_own[t, l, h]
                for j in range(PARTS):
                    acc[l, h, :, j * LANES : (j + 1) * LANES] = rescaled(masked.at[t, l, h], tile, j)

    with jax.named_scope("waitfar"):
        wait(far_in, sem_got.at[FAR])
    with jax.named_scope("waitfarprob"):
        wait(far_prob, sem_got.at[PROB_F])
    for l in range(LAYERS):
        for h in range(2):
            owner = (up, down)[h]
            tile, far_tile = inv_own[owner, l, h], 1.0 / far_prob[h, l].astype(F32)
            for j in range(PARTS):
                joint[h, l, :, j * LANES : (j + 1) * LANES] = (
                    rescaled(masked.at[owner, l, h], tile, j) + rescaled(far_in.at[h, l], far_tile, j)
                ).astype(BF16)
            send(joint.at[h, l], joint_in.at[h, l], None, ENTRIES, at_task(3 if h else 1), sem_j.at[l])

    with jax.named_scope("waitpy"):
        wait(prob_in, sem_got.at[PROB_Y])
    with jax.named_scope("waitraw"):
        wait(raw_in, sem_got.at[NEAR])
    with jax.named_scope("raw"):
        for l in range(LAYERS):
            for h in range(2):
                tile = 1.0 / prob_in[h, l].astype(F32)
                for j in range(PARTS):
                    cols = slice(j * LANES, (j + 1) * LANES)
                    acc[l, h, :, cols] = acc[l, h, :, cols] + rescaled(raw_in.at[h, l], tile, j)
    for l in range(LAYERS):
        with jax.named_scope(f"waitjoint#l={l}"):
            wait(joint_in.at[:, l], sem_j.at[l])
        for h in range(2):
            for j in range(PARTS):
                cols = slice(j * LANES, (j + 1) * LANES)
                out[l, :, h * HALF + j * LANES : h * HALF + (j + 1) * LANES] = (
                    acc[l, h, :, cols] + joint_in[h, l, :, cols].astype(F32)
                ).astype(BF16)

    with jax.named_scope("waitsend"):
        @pl.when(hub)
        def _():
            wait(tot_z, sem_sent.at[TOTALS])

        @pl.when(jnp.logical_not(hub))
        def _():
            wait(tot_z.at[pl.ds(0, 2)], sem_sent.at[TOTALS])

        wait(masked.at[pl.ds(0, 3), 0], sem_sent.at[COLUMNS])
        wait(masked.at[0, 0, 0], sem_sent.at[PROBS])
        wait(masked.at[pl.ds(0, 3)], sem_sent.at[ENTRIES])


def on_device(task_deltas, rank_scores, keep_limits):
    dma = pltpu.SemaphoreType.DMA
    inputs = (pltpu.with_memory_space_constraint(x, pltpu.HBM) for x in (task_deltas, rank_scores, keep_limits))
    return pl.pallas_call(
        kernel,
        out_shape=jax.ShapeDtypeStruct((LAYERS, HERE, 2 * HALF), BF16),
        in_specs=[pl.BlockSpec(memory_space=pl.ANY)] * 3,
        out_specs=pl.BlockSpec(memory_space=pltpu.VMEM),
        scratch_shapes=[
            pltpu.SMEM((1, LAYERS, EXPERTS), jnp.int32),
            pltpu.VMEM((LAYERS, HERE, FF), BF16),
            pltpu.VMEM((LAYERS, HERE, FF), jnp.int32),
            pltpu.VMEM((TASKS, LAYERS, 2, HERE, HALF), BF16),
            pltpu.VMEM((2, TASKS, LAYERS, PARTS, LANES), F32),
            pltpu.VMEM((TASKS, LAYERS, PARTS, LANES), F32),
            *[pltpu.VMEM((TASKS, LAYERS, PARTS, LANES), F32)] * 4,
            pltpu.VMEM((TASKS, LAYERS, 2, PARTS, LANES), BF16),
            pltpu.VMEM((TASKS, LAYERS, 2, PARTS, LANES), F32),
            *[pltpu.VMEM((2, LAYERS, PARTS, LANES), BF16)] * 2,
            pltpu.VMEM((LAYERS, 2, HERE, HALF), F32),
            *[pltpu.VMEM((2, LAYERS, HERE, HALF), BF16)] * 4,
            pltpu.VMEM((8, LANES), F32),
            pltpu.VMEM((2 * GROUP - 1, 8, LANES), F32),
            pltpu.VMEM((8, LANES), F32),
            pltpu.VMEM((3, 8, LANES), F32),
            pltpu.VMEM((8, LANES), F32),
            dma((10,)),
            dma((4,)),
            dma((10,)),
            dma((LAYERS,)),
            pltpu.SemaphoreType.REGULAR,
            pltpu.SemaphoreType.REGULAR,
        ],
        compiler_params=pltpu.CompilerParams(
            collective_id=0, has_side_effects=True, vmem_limit_bytes=32 * 1024 * 1024
        ),
    )(*inputs)


def solution(mesh):
    in_specs = (P("task", None, "shard", None), P("task", None, "shard", None), P("task", None, None))
    return jax.shard_map(on_device, mesh=mesh, in_specs=in_specs, out_specs=P(None, "shard", "task"), check_vma=False)
```

```python
import functools

import jax
import jax.numpy as jnp
from jax import lax
from jax.experimental import pallas as pl
from jax.experimental.pallas import tpu as pltpu
from jax.sharding import PartitionSpec as P

EXPERTS = 8
ROWS = 64
FF = 16384
LAYERS = 4
TASKS = 4
SHARDS = 32
GROUP = 4
HERE = 16
HALF = 2048
LANES = 128
PARTS = HALF // LANES
HELD = 1

MESH = pl.DeviceIdType.MESH
F32 = jnp.float32
BF16 = jnp.bfloat16


def kernel(
    delta, score, limit_in, out,
    limit, dbuf, sbuf, masked, sums, pair_in, chip_out, chip_in, half, half_in, prob, inv_own, prob_in, far_prob, acc, raw_in,
    far_in, joint, joint_in, tot, tot_z, tot_l, tot2, tot_x, tot_f, grand,
    sem_load, sem_sent, sem_got, sem_j, sem_near, sem_line,
):
    s, t = lax.axis_index("shard"), lax.axis_index("task")
    expert = lax.div(s, GROUP)
    member = lax.rem(s, GROUP)
    core = lax.rem(s, 2)
    first = expert * GROUP
    late = lax.rem(expert, 2)
    other = (expert + 1 - 2 * late) * GROUP
    hub = jnp.logical_and(late == 0, core == 1)

    def at_task(d):
        return (s, lax.rem(t + d, TASKS))

    def at_x(d):
        return (lax.rem(s + 2 * GROUP * d, SHARDS), t)

    def at_other(m):
        return (other + m, t)

    def block_of(owner):
        return pl.ds(pl.multiple_of(owner * 2 * HALF, 2 * HALF), 2 * HALF)

    def at_group(d):
        return (first + lax.rem(member + d, GROUP), t)

    def send(src, dst, kind, sent, to, got=None):
        copy = pltpu.make_async_remote_copy(
            src_ref=src, dst_ref=dst, send_sem=sem_sent.at[sent], recv_sem=sem_got.at[kind] if got is None else got,
            device_id=to, device_id_type=MESH,
        )
        copy.start()

    def wait(ref, sem):
        pltpu.make_async_copy(ref, ref, sem).wait()

    PAIR, CHIP, WHOLE, TOTAL, TOTAL_L, TOTAL_X, TOTAL_F, GRAND, PROB_F, PROB_Y, NEAR, FAR = range(12)
    COLUMNS, TOTALS, PROBS, ENTRIES = range(4)

    barrier = pltpu.get_barrier_semaphore()

    def greet(to):
        pl.semaphore_signal(barrier, inc=1, device_id=to, device_id_type=MESH)

    wide = t < 2
    at_x0 = lax.div(s, 2 * GROUP)
    greet(at_task(1))
    greet(at_task(3))
    up, down, far_owner = lax.rem(t + 1, TASKS), lax.rem(t + 3, TASKS), lax.rem(t + 2, TASKS)
    first_d, first_s = delta.at[0, 0], score.at[0, 0]
    pieces = [(limit_in, limit, 0)]
    pieces.append((first_d.at[:, block_of(far_owner)], dbuf.at[0, :, block_of(far_owner)], 1))
    pieces.append((first_s.at[:, block_of(far_owner)], sbuf.at[0, :, block_of(far_owner)], 1))
    for owner in (up, down):
        pieces.append((first_d.at[:, block_of(owner)], dbuf.at[0, :, block_of(owner)], 2))
    pieces.append((first_d.at[:, block_of(t)], dbuf.at[0, :, block_of(t)], 3))
    for l in range(1, LAYERS):
        pieces.append((delta.at[0, l], dbuf.at[l], 3 + l))
    for owner in (up, down):
        pieces.append((first_s.at[:, block_of(owner)], sbuf.at[0, :, block_of(owner)], 7))
    pieces.append((first_s.at[:, block_of(t)], sbuf.at[0, :, block_of(t)], 8))
    pieces.append((score.at[0, pl.ds(1, LAYERS - 1)], sbuf.at[pl.ds(1, LAYERS - 1)], 9))
    loads = [pltpu.make_async_copy(src, dst, sem_load.at[i]) for src, dst, i in pieces]
    for load in loads:
        load.start()

    for d in (1, 2, 3):
        pl.when(jnp.logical_or(wide, member + d < GROUP))(functools.partial(greet, at_group(d)))

    @pl.when(hub)
    def _():
        for d in (1, 2, 3):
            pl.when(jnp.logical_or(wide, at_x0 + d < SHARDS // (2 * GROUP)))(functools.partial(greet, at_x(d)))
        for m in range(GROUP):
            greet(at_other(m))

        @pl.when(at_x0 == 0)
        def _():
            for x in range(1, SHARDS // (2 * GROUP)):
                for m in range(GROUP):
                    greet(((2 * x + 1) * GROUP + m, t))

    place = lax.broadcasted_iota(jnp.int32, (PARTS, PARTS * HERE), 1) - HERE * lax.broadcasted_iota(
        jnp.int32, (PARTS, PARTS * HERE), 0
    )
    pick = jnp.where(jnp.logical_and(place >= 0, place < HERE), F32(1.0), F32(0.0)).astype(BF16)

    def sum_layer(l):
        def body(i, carry):
            b, h = lax.div(i, 2), lax.rem(i, 2)
            blocks = [
                jnp.abs(dbuf[l, :, pl.ds(pl.multiple_of(i * HALF + j * LANES, LANES), LANES)]) for j in range(PARTS)
            ]
            sums[h, b, l] = jnp.dot(pick, jnp.concatenate(blocks, axis=0), preferred_element_type=F32)
            return carry

        lax.fori_loop(0, 2 * TASKS, body, 0, unroll=True)

    def mask_half(l, i):
        b, h = lax.div(i, 2), lax.rem(i, 2)
        own_limit = limit[0, l, expert]
        for j in range(PARTS):
            cols = pl.ds(pl.multiple_of(i * HALF + j * LANES, LANES), LANES)
            keep = sbuf[l, :, cols] < own_limit
            masked[b, l, h, :, j * LANES : (j + 1) * LANES] = jnp.where(
                keep, dbuf[l, :, cols].astype(F32), F32(0.0)
            ).astype(BF16)

    def mask_block(l, owner):
        def body(i, carry):
            mask_half(l, 2 * owner + i)
            return carry

        lax.fori_loop(0, 2, body, 0)

    def mask_layer(l):
        def body(i, carry):
            mask_half(l, i)
            return carry

        lax.fori_loop(0, 2 * TASKS, body, 0)

    def send_far(l):
        for h in range(2):
            send(masked.at[far_owner, l, h], far_in.at[h, l], FAR, ENTRIES, at_task(3 if h else 1))

    def send_near(l):
        for d, owner, h in ((1, up, 1), (3, down, 0)):
            send(masked.at[owner, l, h], raw_in.at[h, l], NEAR, ENTRIES, at_task(d))

    with jax.named_scope("load"):
        loads[0].wait()
        wait(sbuf.at[0, :, pl.ds(0, 3 * HALF)], sem_load.at[1])
    with jax.named_scope("mask0"):
        mask_block(0, far_owner)

    def all_sums():
        wait(dbuf.at[0, :, pl.ds(0, 4 * HALF)], sem_load.at[2])
        for l in range(LAYERS):
            wait(dbuf.at[l] if l else dbuf.at[0, :, pl.ds(0, 2 * HALF)], sem_load.at[3 + l])
            sum_layer(l)

    def mask_near():
        wait(sbuf.at[0, :, pl.ds(0, 4 * HALF)], sem_load.at[7])
        mask_block(0, up)
        mask_block(0, down)

    with jax.named_scope("sums0"):

        @pl.when(t < 2)
        def _():
            all_sums()
            mask_near()

    with jax.named_scope("bar"):
        met = jnp.where(wide, GROUP - 1, member) + 2 * late * jnp.where(at_x0 > 0, 2, 1) + jnp.where(hub, jnp.where(wide, GROUP - 1, at_x0), 0)
        pl.semaphore_wait(barrier, 2 + met)
    send_far(0)

    @pl.when(jnp.logical_not(wide))
    def _():
        for d in (1, 2, 3):
            for back, peer, sem in (
                (member - d >= 0, at_group(4 - d), sem_near),
                (jnp.logical_and(hub, at_x0 - d >= 0), at_x(4 - d), sem_line),
            ):

                @pl.when(back)
                def _():
                    pl.semaphore_signal(sem, inc=1, device_id=peer, device_id_type=MESH)

    with jax.named_scope("sums1"):

        @pl.when(t >= 2)
        def _():
            all_sums()
            mask_near()

    send_near(0)

    for l in range(LAYERS):
        whole = sums[0, 0, l] + sums[1, 0, l]
        for b in range(1, TASKS):
            whole = whole + sums[0, b, l] + sums[1, b, l]
        tot[l : l + 1, :] = jnp.sum(whole, axis=0, keepdims=True)
    tot[LAYERS:, :] = jnp.zeros((8 - LAYERS, LANES), F32)

    @pl.when(late == 1)
    def _():
        for m in (1, 3):
            send(tot, tot_l.at[member], TOTAL_L, TOTALS, at_other(m))

        @pl.when(at_x0 > 0)
        def _():
            for m in (1, 3):
                send(tot, tot_f.at[GROUP * (at_x0 - 1) + member], TOTAL_F, TOTALS, (m, t))

    with jax.named_scope("near"):

        to_come = GROUP - 1 - member

        @pl.when(jnp.logical_and(jnp.logical_not(wide), to_come > 0))
        def _():
            pl.semaphore_wait(sem_near, to_come)

    send(sums.at[1 - core], pair_in, PAIR, COLUMNS, at_group(1 - 2 * core + GROUP))

    @pl.when(late == 0)
    def _():
        for d in range(1, GROUP):
            pl.when(lax.rem(member + d, 2) == 1)(
                functools.partial(send, tot, tot_z.at[d - 1], TOTAL, TOTALS, at_group(d))
            )

    with jax.named_scope("masks"):
        wait(sbuf.at[0, :, pl.ds(0, 2 * HALF)], sem_load.at[8])
        mask_block(0, t)
        wait(sbuf.at[pl.ds(1, LAYERS - 1)], sem_load.at[9])
        for l in range(1, LAYERS):
            mask_layer(l)
            send_far(l)
        for l in range(1, LAYERS - HELD):
            send_near(l)

    with jax.named_scope("waitpair"):
        wait(pair_in, sem_got.at[PAIR])
    half[...] = sums[core] + pair_in[...]
    chip_out[...] = half[...]
    send(chip_out, chip_in, CHIP, COLUMNS, at_group(2))

    with jax.named_scope("totals1"):

        @pl.when(hub)
        def _():
            to_come_x = GROUP - 1 - at_x0

            @pl.when(jnp.logical_and(jnp.logical_not(wide), to_come_x > 0))
            def _():
                pl.semaphore_wait(sem_line, to_come_x)

            wait(tot_z, sem_got.at[TOTAL])
            early = tot[...] + tot_z[0] + tot_z[1] + tot_z[2]
            tot2[0] = early

            @pl.when(at_x0 > 0)
            def _():
                send(tot2.at[0], tot_x.at[3 - at_x0], TOTAL_X, TOTALS, (member, t))

            wait(tot_l, sem_got.at[TOTAL_L])
            tot2[1] = early + tot_l[0] + tot_l[1] + tot_l[2] + tot_l[3]
            for d in (1, 2, 3):

                @pl.when(at_x0 + d != SHARDS // (2 * GROUP))
                def _():
                    send(tot2.at[1], tot_x.at[d - 1], TOTAL_X, TOTALS, at_x(d))

    with jax.named_scope("waitchip"):
        wait(chip_in, sem_got.at[CHIP])
    half[...] = chip_out[...] + chip_in[...]
    send(half, half_in, WHOLE, COLUMNS, at_group(1 - 2 * core + GROUP))
    with jax.named_scope("totals2"):

        @pl.when(hub)
        def _():
            wait(tot_x, sem_got.at[TOTAL_X])
            grand[...] = tot2[1] + tot_x[0] + tot_x[1] + tot_x[2]

            @pl.when(at_x0 == 0)
            def _():
                wait(tot_f, sem_got.at[TOTAL_F])
                whole = grand[...]
                for i in range(3 * GROUP):
                    whole = whole + tot_f[i]
                grand[...] = whole

            send(grand, grand, GRAND, TOTALS, at_other(GROUP - 1 - member))
            send(grand, grand, GRAND, TOTALS, at_other(GROUP - member))
            send(grand, grand, GRAND, TOTALS, at_group(GROUP - 1))

        @pl.when(jnp.logical_not(hub))
        def _():
            wait(grand, sem_got.at[GRAND])

    grand_mean = jnp.sum(grand[...], axis=1, keepdims=True) / F32(EXPERTS * ROWS * FF)
    with jax.named_scope("waitwhole"):
        wait(half_in, sem_got.at[WHOLE])

    def make_prob(b, l):
        mean_l = jnp.broadcast_to(grand_mean[l : l + 1, :], (PARTS, LANES))
        mine, theirs = half[b, l], half_in[b, l]
        for h in range(2):
            column = jnp.where(core == h, mine, theirs) / F32(ROWS)
            rounded = (0.2 + 0.7 * column / (column + mean_l)).astype(BF16)
            prob[b, l, h] = rounded
            inv_own[b, l, h] = 1.0 / rounded.astype(F32)

    def rescaled(block, tile, j):
        return block[:, j * LANES : (j + 1) * LANES].astype(F32) * tile[j : j + 1, :]

    with jax.named_scope("farprob"):
        for l in range(LAYERS):
            make_prob(far_owner, l)
        for h in range(2):
            send(prob.at[far_owner, :, h], far_prob.at[h], PROB_F, PROBS, at_task(3 if h else 1))
    with jax.named_scope("prob"):
        for owner in (up, down, t):
            for l in range(LAYERS):
                make_prob(owner, l)
    for l in range(LAYERS - HELD, LAYERS):
        send_near(l)
    for d, owner, h in ((1, up, 1), (3, down, 0)):
        send(prob.at[owner, :, h], prob_in.at[h], PROB_Y, PROBS, at_task(d))

    with jax.named_scope("own"):
        for l in range(LAYERS):
            for h in range(2):
                tile = inv_own[t, l, h]
                for j in range(PARTS):
                    acc[l, h, :, j * LANES : (j + 1) * LANES] = rescaled(masked.at[t, l, h], tile, j)

    with jax.named_scope("waitfar"):
        wait(far_in, sem_got.at[FAR])
    with jax.named_scope("waitfarprob"):
        wait(far_prob, sem_got.at[PROB_F])
    for l in range(LAYERS):
        for h in range(2):
            owner = (up, down)[h]
            tile, far_tile = inv_own[owner, l, h], 1.0 / far_prob[h, l].astype(F32)
            for j in range(PARTS):
                joint[h, l, :, j * LANES : (j + 1) * LANES] = (
                    rescaled(masked.at[owner, l, h], tile, j) + rescaled(far_in.at[h, l], far_tile, j)
                ).astype(BF16)
            send(joint.at[h, l], joint_in.at[h, l], None, ENTRIES, at_task(3 if h else 1), sem_j.at[l])

    with jax.named_scope("waitpy"):
        wait(prob_in, sem_got.at[PROB_Y])
    with jax.named_scope("waitraw"):
        wait(raw_in, sem_got.at[NEAR])
    with jax.named_scope("raw"):
        for l in range(LAYERS):
            for h in range(2):
                tile = 1.0 / prob_in[h, l].astype(F32)
                for j in range(PARTS):
                    cols = slice(j * LANES, (j + 1) * LANES)
                    acc[l, h, :, cols] = acc[l, h, :, cols] + rescaled(raw_in.at[h, l], tile, j)
    for l in range(LAYERS):
        with jax.named_scope(f"waitjoint#l={l}"):
            wait(joint_in.at[:, l], sem_j.at[l])
        for h in range(2):
            for j in range(PARTS):
                cols = slice(j * LANES, (j + 1) * LANES)
                out[l, :, h * HALF + j * LANES : h * HALF + (j + 1) * LANES] = (
                    acc[l, h, :, cols] + joint_in[h, l, :, cols].astype(F32)
                ).astype(BF16)

    with jax.named_scope("waitsend"):
        @pl.when(hub)
        def _():
            wait(tot_f.at[pl.ds(0, 7)], sem_sent.at[TOTALS])

        direct = jnp.logical_and(late == 1, at_x0 > 0)

        @pl.when(direct)
        def _():
            wait(tot_f.at[pl.ds(0, 4)], sem_sent.at[TOTALS])

        @pl.when(jnp.logical_not(jnp.logical_or(hub, direct)))
        def _():
            wait(tot_f.at[pl.ds(0, 2)], sem_sent.at[TOTALS])

        wait(masked.at[pl.ds(0, 3), 0], sem_sent.at[COLUMNS])
        wait(masked.at[0, 0, 0], sem_sent.at[PROBS])
        wait(masked.at[pl.ds(0, 3)], sem_sent.at[ENTRIES])


def on_device(task_deltas, rank_scores, keep_limits):
    dma = pltpu.SemaphoreType.DMA
    inputs = (pltpu.with_memory_space_constraint(x, pltpu.HBM) for x in (task_deltas, rank_scores, keep_limits))
    return pl.pallas_call(
        kernel,
        out_shape=jax.ShapeDtypeStruct((LAYERS, HERE, 2 * HALF), BF16),
        in_specs=[pl.BlockSpec(memory_space=pl.ANY)] * 3,
        out_specs=pl.BlockSpec(memory_space=pltpu.VMEM),
        scratch_shapes=[
            pltpu.SMEM((1, LAYERS, EXPERTS), jnp.int32),
            pltpu.VMEM((LAYERS, HERE, FF), BF16),
            pltpu.VMEM((LAYERS, HERE, FF), jnp.int32),
            pltpu.VMEM((TASKS, LAYERS, 2, HERE, HALF), BF16),
            pltpu.VMEM((2, TASKS, LAYERS, PARTS, LANES), F32),
            pltpu.VMEM((TASKS, LAYERS, PARTS, LANES), F32),
            *[pltpu.VMEM((TASKS, LAYERS, PARTS, LANES), F32)] * 4,
            pltpu.VMEM((TASKS, LAYERS, 2, PARTS, LANES), BF16),
            pltpu.VMEM((TASKS, LAYERS, 2, PARTS, LANES), F32),
            *[pltpu.VMEM((2, LAYERS, PARTS, LANES), BF16)] * 2,
            pltpu.VMEM((LAYERS, 2, HERE, HALF), F32),
            *[pltpu.VMEM((2, LAYERS, HERE, HALF), BF16)] * 4,
            pltpu.VMEM((8, LANES), F32),
            pltpu.VMEM((GROUP - 1, 8, LANES), F32),
            pltpu.VMEM((GROUP, 8, LANES), F32),
            pltpu.VMEM((2, 8, LANES), F32),
            pltpu.VMEM((3, 8, LANES), F32),
            pltpu.VMEM((3 * GROUP, 8, LANES), F32),
            pltpu.VMEM((8, LANES), F32),
            dma((10,)),
            dma((4,)),
            dma((12,)),
            dma((LAYERS,)),
            pltpu.SemaphoreType.REGULAR,
            pltpu.SemaphoreType.REGULAR,
        ],
        compiler_params=pltpu.CompilerParams(
            collective_id=0, has_side_effects=True, vmem_limit_bytes=32 * 1024 * 1024
        ),
    )(*inputs)


def solution(mesh):
    in_specs = (P("task", None, "shard", None), P("task", None, "shard", None), P("task", None, None))
    return jax.shard_map(on_device, mesh=mesh, in_specs=in_specs, out_specs=P(None, "shard", "task"), check_vma=False)
```

```python
import functools

import jax
import jax.numpy as jnp
from jax import lax
from jax.experimental import pallas as pl
from jax.experimental.pallas import tpu as pltpu
from jax.sharding import PartitionSpec as P

EXPERTS = 8
ROWS = 64
FF = 16384
LAYERS = 4
TASKS = 4
SHARDS = 32
GROUP = 4
LINE = 4
HERE = 16
HALF = 2048
LANES = 128
PARTS = HALF // LANES
HELD = 1

MESH = pl.DeviceIdType.MESH
F32 = jnp.float32
BF16 = jnp.bfloat16


def kernel(
    delta, score, limit_in, out,
    limit, dbuf, sbuf, masked, sums, pair_in, chip_out, chip_in, half, half_in, prob, inv_own, prob_in, far_prob, acc, raw_in,
    far_in, joint, joint_in, tot, tot_z, tot_l, tot2, tot_x, tot_f, grand,
    sem_load, sem_sent, sem_got, sem_j, sem_near, sem_line,
):
    s, t = lax.axis_index("shard"), lax.axis_index("task")
    expert = lax.div(s, GROUP)
    member = lax.rem(s, GROUP)
    core = lax.rem(s, 2)
    first = expert * GROUP
    late = lax.rem(expert, 2)
    other = (expert + 1 - 2 * late) * GROUP
    hub = jnp.logical_and(late == 0, core == 1)

    def at_task(d):
        return (s, lax.rem(t + d, TASKS))

    def at_x(d):
        return (lax.rem(s + 2 * GROUP * d, SHARDS), t)

    def at_other(m):
        return (other + m, t)

    def block_of(owner):
        return pl.ds(pl.multiple_of(owner * 2 * HALF, 2 * HALF), 2 * HALF)

    def at_group(d):
        return (first + lax.rem(member + d, GROUP), t)

    def send(src, dst, kind, sent, to, got=None):
        copy = pltpu.make_async_remote_copy(
            src_ref=src, dst_ref=dst, send_sem=sem_sent.at[sent], recv_sem=sem_got.at[kind] if got is None else got,
            device_id=to, device_id_type=MESH,
        )
        copy.start()

    def wait(ref, sem):
        pltpu.make_async_copy(ref, ref, sem).wait()

    PAIR, CHIP, WHOLE, TOTAL, TOTAL_L, TOTAL_X, TOTAL_F, GRAND, PROB_F, PROB_Y, NEAR, FAR = range(12)
    COLUMNS, TOTALS, PROBS, ENTRIES = range(4)

    barrier = pltpu.get_barrier_semaphore()

    def greet(to):
        pl.semaphore_signal(barrier, inc=1, device_id=to, device_id_type=MESH)

    wide = t < 2
    at_x0 = lax.div(s, 2 * GROUP)
    greet(at_task(1))
    greet(at_task(3))
    up, down, far_owner = lax.rem(t + 1, TASKS), lax.rem(t + 3, TASKS), lax.rem(t + 2, TASKS)
    first_d, first_s = delta.at[0, 0], score.at[0, 0]
    pieces = [(limit_in, limit, 0)]
    pieces.append((first_d.at[:, block_of(far_owner)], dbuf.at[0, :, block_of(far_owner)], 1))
    pieces.append((first_s.at[:, block_of(far_owner)], sbuf.at[0, :, block_of(far_owner)], 1))
    for owner in (up, down):
        pieces.append((first_d.at[:, block_of(owner)], dbuf.at[0, :, block_of(owner)], 2))
    pieces.append((first_d.at[:, block_of(t)], dbuf.at[0, :, block_of(t)], 3))
    for l in range(1, LAYERS):
        pieces.append((delta.at[0, l], dbuf.at[l], 3 + l))
    for owner in (up, down):
        pieces.append((first_s.at[:, block_of(owner)], sbuf.at[0, :, block_of(owner)], 7))
    pieces.append((first_s.at[:, block_of(t)], sbuf.at[0, :, block_of(t)], 8))
    pieces.append((score.at[0, pl.ds(1, LAYERS - 1)], sbuf.at[pl.ds(1, LAYERS - 1)], 9))
    loads = [pltpu.make_async_copy(src, dst, sem_load.at[i]) for src, dst, i in pieces]
    for load in loads:
        load.start()

    for d in (1, 2, 3):
        pl.when(jnp.logical_or(wide, member + d < GROUP))(functools.partial(greet, at_group(d)))

    @pl.when(hub)
    def _():
        for d in (1, 2, 3):
            pl.when(jnp.logical_or(wide, at_x0 + d < LINE))(functools.partial(greet, at_x(d)))
        for m in range(GROUP):
            greet(at_other(m))

        for x in range(1, LINE):

            @pl.when(at_x0 < x)
            def _():
                for m in range(GROUP):
                    greet(((2 * x + 1) * GROUP + m, t))

    place = lax.broadcasted_iota(jnp.int32, (PARTS, PARTS * HERE), 1) - HERE * lax.broadcasted_iota(
        jnp.int32, (PARTS, PARTS * HERE), 0
    )
    pick = jnp.where(jnp.logical_and(place >= 0, place < HERE), F32(1.0), F32(0.0)).astype(BF16)

    def sum_layer(l):
        def body(i, carry):
            b, h = lax.div(i, 2), lax.rem(i, 2)
            blocks = [
                jnp.abs(dbuf[l, :, pl.ds(pl.multiple_of(i * HALF + j * LANES, LANES), LANES)]) for j in range(PARTS)
            ]
            sums[h, b, l] = jnp.dot(pick, jnp.concatenate(blocks, axis=0), preferred_element_type=F32)
            return carry

        lax.fori_loop(0, 2 * TASKS, body, 0, unroll=True)

    def mask_half(l, i):
        b, h = lax.div(i, 2), lax.rem(i, 2)
        own_limit = limit[0, l, expert]
        for j in range(PARTS):
            cols = pl.ds(pl.multiple_of(i * HALF + j * LANES, LANES), LANES)
            keep = sbuf[l, :, cols] < own_limit
            masked[b, l, h, :, j * LANES : (j + 1) * LANES] = jnp.where(
                keep, dbuf[l, :, cols].astype(F32), F32(0.0)
            ).astype(BF16)

    def mask_block(l, owner):
        def body(i, carry):
            mask_half(l, 2 * owner + i)
            return carry

        lax.fori_loop(0, 2, body, 0)

    def mask_layer(l):
        def body(i, carry):
            mask_half(l, i)
            return carry

        lax.fori_loop(0, 2 * TASKS, body, 0)

    def send_far(l):
        for h in range(2):
            send(masked.at[far_owner, l, h], far_in.at[h, l], FAR, ENTRIES, at_task(3 if h else 1))

    def send_near(l):
        for d, owner, h in ((1, up, 1), (3, down, 0)):
            send(masked.at[owner, l, h], raw_in.at[h, l], NEAR, ENTRIES, at_task(d))

    with jax.named_scope("load"):
        loads[0].wait()
        wait(sbuf.at[0, :, pl.ds(0, 3 * HALF)], sem_load.at[1])
    with jax.named_scope("mask0"):
        mask_block(0, far_owner)

    def all_sums():
        wait(dbuf.at[0, :, pl.ds(0, 4 * HALF)], sem_load.at[2])
        for l in range(LAYERS):
            wait(dbuf.at[l] if l else dbuf.at[0, :, pl.ds(0, 2 * HALF)], sem_load.at[3 + l])
            sum_layer(l)

    def mask_near():
        wait(sbuf.at[0, :, pl.ds(0, 4 * HALF)], sem_load.at[7])
        mask_block(0, up)
        mask_block(0, down)

    with jax.named_scope("sums0"):

        @pl.when(t < 2)
        def _():
            all_sums()
            mask_near()

    with jax.named_scope("bar"):
        met = jnp.where(wide, GROUP - 1, member) + 2 * late * (1 + at_x0) + jnp.where(hub, jnp.where(wide, GROUP - 1, at_x0), 0)
        pl.semaphore_wait(barrier, 2 + met)
    send_far(0)

    @pl.when(jnp.logical_not(wide))
    def _():
        for d in (1, 2, 3):
            for back, peer, sem in (
                (member - d >= 0, at_group(4 - d), sem_near),
                (jnp.logical_and(hub, at_x0 - d >= 0), at_x(4 - d), sem_line),
            ):

                @pl.when(back)
                def _():
                    pl.semaphore_signal(sem, inc=1, device_id=peer, device_id_type=MESH)

    with jax.named_scope("sums1"):

        @pl.when(t >= 2)
        def _():
            all_sums()
            mask_near()

    send_near(0)

    for l in range(LAYERS):
        whole = sums[0, 0, l] + sums[1, 0, l]
        for b in range(1, TASKS):
            whole = whole + sums[0, b, l] + sums[1, b, l]
        tot[l : l + 1, :] = jnp.sum(whole, axis=0, keepdims=True)
    tot[LAYERS:, :] = jnp.zeros((8 - LAYERS, LANES), F32)

    @pl.when(late == 1)
    def _():
        for m in (1, 3):
            send(tot, tot_l.at[member], TOTAL_L, TOTALS, at_other(m))

        for x in range(LINE - 1):

            @pl.when(at_x0 > x)
            def _():
                for m in (1, 3):
                    slot = GROUP * (at_x0 - x - 1) + member
                    send(tot, tot_f.at[slot], TOTAL_F, TOTALS, (2 * GROUP * x + m, t))

    with jax.named_scope("near"):

        to_come = GROUP - 1 - member

        @pl.when(jnp.logical_and(jnp.logical_not(wide), to_come > 0))
        def _():
            pl.semaphore_wait(sem_near, to_come)

    send(sums.at[1 - core], pair_in, PAIR, COLUMNS, at_group(1 - 2 * core + GROUP))

    @pl.when(late == 0)
    def _():
        for d in range(1, GROUP):
            pl.when(lax.rem(member + d, 2) == 1)(
                functools.partial(send, tot, tot_z.at[d - 1], TOTAL, TOTALS, at_group(d))
            )

    with jax.named_scope("masks"):
        wait(sbuf.at[0, :, pl.ds(0, 2 * HALF)], sem_load.at[8])
        mask_block(0, t)
        wait(sbuf.at[pl.ds(1, LAYERS - 1)], sem_load.at[9])
        for l in range(1, LAYERS):
            mask_layer(l)
            send_far(l)
        for l in range(1, LAYERS - HELD):
            send_near(l)

    with jax.named_scope("waitpair"):
        wait(pair_in, sem_got.at[PAIR])
    half[...] = sums[core] + pair_in[...]
    chip_out[...] = half[...]
    send(chip_out, chip_in, CHIP, COLUMNS, at_group(2))

    with jax.named_scope("totals1"):

        @pl.when(hub)
        def _():
            to_come_x = GROUP - 1 - at_x0

            @pl.when(jnp.logical_and(jnp.logical_not(wide), to_come_x > 0))
            def _():
                pl.semaphore_wait(sem_line, to_come_x)

            wait(tot_z, sem_got.at[TOTAL])
            early = tot[...] + tot_z[0] + tot_z[1] + tot_z[2]
            tot2[0] = early

            for d in (1, 2, 3):

                @pl.when(at_x0 + d >= LINE)
                def _():
                    send(tot2.at[0], tot_x.at[d - 1], TOTAL_X, TOTALS, at_x(d))

            wait(tot_l, sem_got.at[TOTAL_L])
            tot2[1] = early + tot_l[0] + tot_l[1] + tot_l[2] + tot_l[3]
            for d in (1, 2, 3):

                @pl.when(at_x0 + d < LINE)
                def _():
                    send(tot2.at[1], tot_x.at[d - 1], TOTAL_X, TOTALS, at_x(d))

    with jax.named_scope("waitchip"):
        wait(chip_in, sem_got.at[CHIP])
    half[...] = chip_out[...] + chip_in[...]
    send(half, half_in, WHOLE, COLUMNS, at_group(1 - 2 * core + GROUP))
    with jax.named_scope("totals2"):

        @pl.when(hub)
        def _():
            wait(tot_x, sem_got.at[TOTAL_X])
            grand[...] = tot2[1] + tot_x[0] + tot_x[1] + tot_x[2]

            for x in range(LINE - 1):

                @pl.when(at_x0 == x)
                def _():
                    count = GROUP * (LINE - 1 - x)
                    wait(tot_f.at[pl.ds(0, count)], sem_got.at[TOTAL_F])
                    whole = grand[...]
                    for i in range(count):
                        whole = whole + tot_f[i]
                    grand[...] = whole

            send(grand, grand, GRAND, TOTALS, at_other(GROUP - 1 - member))
            send(grand, grand, GRAND, TOTALS, at_other(GROUP - member))
            send(grand, grand, GRAND, TOTALS, at_group(GROUP - 1))

        @pl.when(jnp.logical_not(hub))
        def _():
            wait(grand, sem_got.at[GRAND])

    grand_mean = jnp.sum(grand[...], axis=1, keepdims=True) / F32(EXPERTS * ROWS * FF)
    with jax.named_scope("waitwhole"):
        wait(half_in, sem_got.at[WHOLE])

    def make_prob(b, l):
        mean_l = jnp.broadcast_to(grand_mean[l : l + 1, :], (PARTS, LANES))
        mine, theirs = half[b, l], half_in[b, l]
        for h in range(2):
            column = jnp.where(core == h, mine, theirs) / F32(ROWS)
            rounded = (0.2 + 0.7 * column / (column + mean_l)).astype(BF16)
            prob[b, l, h] = rounded
            inv_own[b, l, h] = 1.0 / rounded.astype(F32)

    def rescaled(block, tile, j):
        return block[:, j * LANES : (j + 1) * LANES].astype(F32) * tile[j : j + 1, :]

    with jax.named_scope("farprob"):
        for l in range(LAYERS):
            make_prob(far_owner, l)
        for h in range(2):
            send(prob.at[far_owner, :, h], far_prob.at[h], PROB_F, PROBS, at_task(3 if h else 1))
    with jax.named_scope("prob"):
        for owner in (up, down, t):
            for l in range(LAYERS):
                make_prob(owner, l)
    for l in range(LAYERS - HELD, LAYERS):
        send_near(l)
    for d, owner, h in ((1, up, 1), (3, down, 0)):
        send(prob.at[owner, :, h], prob_in.at[h], PROB_Y, PROBS, at_task(d))

    with jax.named_scope("own"):
        for l in range(LAYERS):
            for h in range(2):
                tile = inv_own[t, l, h]
                for j in range(PARTS):
                    acc[l, h, :, j * LANES : (j + 1) * LANES] = rescaled(masked.at[t, l, h], tile, j)

    with jax.named_scope("waitfar"):
        wait(far_in, sem_got.at[FAR])
    with jax.named_scope("waitfarprob"):
        wait(far_prob, sem_got.at[PROB_F])
    for l in range(LAYERS):
        for h in range(2):
            owner = (up, down)[h]
            tile, far_tile = inv_own[owner, l, h], 1.0 / far_prob[h, l].astype(F32)
            for j in range(PARTS):
                joint[h, l, :, j * LANES : (j + 1) * LANES] = (
                    rescaled(masked.at[owner, l, h], tile, j) + rescaled(far_in.at[h, l], far_tile, j)
                ).astype(BF16)
            send(joint.at[h, l], joint_in.at[h, l], None, ENTRIES, at_task(3 if h else 1), sem_j.at[l])

    with jax.named_scope("waitpy"):
        wait(prob_in, sem_got.at[PROB_Y])
    with jax.named_scope("waitraw"):
        wait(raw_in, sem_got.at[NEAR])
    with jax.named_scope("raw"):
        for l in range(LAYERS):
            for h in range(2):
                tile = 1.0 / prob_in[h, l].astype(F32)
                for j in range(PARTS):
                    cols = slice(j * LANES, (j + 1) * LANES)
                    acc[l, h, :, cols] = acc[l, h, :, cols] + rescaled(raw_in.at[h, l], tile, j)
    for l in range(LAYERS):
        with jax.named_scope(f"waitjoint#l={l}"):
            wait(joint_in.at[:, l], sem_j.at[l])
        for h in range(2):
            for j in range(PARTS):
                cols = slice(j * LANES, (j + 1) * LANES)
                out[l, :, h * HALF + j * LANES : h * HALF + (j + 1) * LANES] = (
                    acc[l, h, :, cols] + joint_in[h, l, :, cols].astype(F32)
                ).astype(BF16)

    with jax.named_scope("waitsend"):
        @pl.when(hub)
        def _():
            wait(tot_f.at[pl.ds(0, 7)], sem_sent.at[TOTALS])

        for x in range(LINE):

            @pl.when(jnp.logical_and(late == 1, at_x0 == x))
            def _():
                wait(tot_f.at[pl.ds(0, 2 * (x + 1))], sem_sent.at[TOTALS])

        @pl.when(jnp.logical_and(late == 0, core == 0))
        def _():
            wait(tot_f.at[pl.ds(0, 2)], sem_sent.at[TOTALS])

        wait(masked.at[pl.ds(0, 3), 0], sem_sent.at[COLUMNS])
        wait(masked.at[0, 0, 0], sem_sent.at[PROBS])
        wait(masked.at[pl.ds(0, 3)], sem_sent.at[ENTRIES])


def on_device(task_deltas, rank_scores, keep_limits):
    dma = pltpu.SemaphoreType.DMA
    inputs = (pltpu.with_memory_space_constraint(x, pltpu.HBM) for x in (task_deltas, rank_scores, keep_limits))
    return pl.pallas_call(
        kernel,
        out_shape=jax.ShapeDtypeStruct((LAYERS, HERE, 2 * HALF), BF16),
        in_specs=[pl.BlockSpec(memory_space=pl.ANY)] * 3,
        out_specs=pl.BlockSpec(memory_space=pltpu.VMEM),
        scratch_shapes=[
            pltpu.SMEM((1, LAYERS, EXPERTS), jnp.int32),
            pltpu.VMEM((LAYERS, HERE, FF), BF16),
            pltpu.VMEM((LAYERS, HERE, FF), jnp.int32),
            pltpu.VMEM((TASKS, LAYERS, 2, HERE, HALF), BF16),
            pltpu.VMEM((2, TASKS, LAYERS, PARTS, LANES), F32),
            pltpu.VMEM((TASKS, LAYERS, PARTS, LANES), F32),
            *[pltpu.VMEM((TASKS, LAYERS, PARTS, LANES), F32)] * 4,
            pltpu.VMEM((TASKS, LAYERS, 2, PARTS, LANES), BF16),
            pltpu.VMEM((TASKS, LAYERS, 2, PARTS, LANES), F32),
            *[pltpu.VMEM((2, LAYERS, PARTS, LANES), BF16)] * 2,
            pltpu.VMEM((LAYERS, 2, HERE, HALF), F32),
            *[pltpu.VMEM((2, LAYERS, HERE, HALF), BF16)] * 4,
            pltpu.VMEM((8, LANES), F32),
            pltpu.VMEM((GROUP - 1, 8, LANES), F32),
            pltpu.VMEM((GROUP, 8, LANES), F32),
            pltpu.VMEM((2, 8, LANES), F32),
            pltpu.VMEM((3, 8, LANES), F32),
            pltpu.VMEM((3 * GROUP, 8, LANES), F32),
            pltpu.VMEM((8, LANES), F32),
            dma((10,)),
            dma((4,)),
            dma((12,)),
            dma((LAYERS,)),
            pltpu.SemaphoreType.REGULAR,
            pltpu.SemaphoreType.REGULAR,
        ],
        compiler_params=pltpu.CompilerParams(
            collective_id=0, has_side_effects=True, vmem_limit_bytes=32 * 1024 * 1024
        ),
    )(*inputs)


def solution(mesh):
    in_specs = (P("task", None, "shard", None), P("task", None, "shard", None), P("task", None, None))
    return jax.shard_map(on_device, mesh=mesh, in_specs=in_specs, out_specs=P(None, "shard", "task"), check_vma=False)
```

```python
import functools

import jax
import jax.numpy as jnp
from jax import lax
from jax.experimental import pallas as pl
from jax.experimental.pallas import tpu as pltpu
from jax.sharding import PartitionSpec as P

EXPERTS = 8
ROWS = 64
FF = 16384
LAYERS = 4
TASKS = 4
SHARDS = 32
GROUP = 4
LINE = 4
HERE = 16
HALF = 2048
LANES = 128
PARTS = HALF // LANES
HELD = 1

MESH = pl.DeviceIdType.MESH
F32 = jnp.float32
BF16 = jnp.bfloat16


def kernel(
    delta, score, limit_in, out,
    limit, dbuf, sbuf, masked, sums, pair_in, chip_out, chip_in, half, half_in, prob, inv_own, prob_in, far_prob, acc, raw_in,
    far_in, joint, joint_in, tot, tot_z, tot_l, tot2, tot_x, tot_f, grand,
    sem_load, sem_sent, sem_got, sem_j, sem_near, sem_line,
):
    s, t = lax.axis_index("shard"), lax.axis_index("task")
    expert = lax.div(s, GROUP)
    member = lax.rem(s, GROUP)
    core = lax.rem(s, 2)
    first = expert * GROUP
    late = lax.rem(expert, 2)
    other = (expert + 1 - 2 * late) * GROUP
    hub = jnp.logical_and(late == 0, core == 1)

    def at_task(d):
        return (s, lax.rem(t + d, TASKS))

    def at_x(d):
        return (lax.rem(s + 2 * GROUP * d, SHARDS), t)

    def at_other(m):
        return (other + m, t)

    def block_of(owner):
        return pl.ds(pl.multiple_of(owner * 2 * HALF, 2 * HALF), 2 * HALF)

    def at_group(d):
        return (first + lax.rem(member + d, GROUP), t)

    def send(src, dst, kind, sent, to, got=None):
        copy = pltpu.make_async_remote_copy(
            src_ref=src, dst_ref=dst, send_sem=sem_sent.at[sent], recv_sem=sem_got.at[kind] if got is None else got,
            device_id=to, device_id_type=MESH,
        )
        copy.start()

    def wait(ref, sem):
        pltpu.make_async_copy(ref, ref, sem).wait()

    PAIR, CHIP, WHOLE, TOTAL, TOTAL_L, TOTAL_X, TOTAL_F, GRAND, PROB_F, PROB_Y, PROB_P, NEAR, FAR = range(13)
    COLUMNS, TOTALS, PROBS, ENTRIES = range(4)

    barrier = pltpu.get_barrier_semaphore()

    def greet(to):
        pl.semaphore_signal(barrier, inc=1, device_id=to, device_id_type=MESH)

    wide = t < 2
    at_x0 = lax.div(s, 2 * GROUP)
    greet(at_task(1))
    greet(at_task(3))
    up, down, far_owner = lax.rem(t + 1, TASKS), lax.rem(t + 3, TASKS), lax.rem(t + 2, TASKS)
    first_d, first_s = delta.at[0, 0], score.at[0, 0]
    pieces = [(limit_in, limit, 0)]
    pieces.append((first_d.at[:, block_of(far_owner)], dbuf.at[0, :, block_of(far_owner)], 1))
    pieces.append((first_s.at[:, block_of(far_owner)], sbuf.at[0, :, block_of(far_owner)], 1))
    for owner in (up, down):
        pieces.append((first_d.at[:, block_of(owner)], dbuf.at[0, :, block_of(owner)], 2))
    pieces.append((first_d.at[:, block_of(t)], dbuf.at[0, :, block_of(t)], 3))
    for l in range(1, LAYERS):
        pieces.append((delta.at[0, l], dbuf.at[l], 3 + l))
    for owner in (up, down):
        pieces.append((first_s.at[:, block_of(owner)], sbuf.at[0, :, block_of(owner)], 7))
    pieces.append((first_s.at[:, block_of(t)], sbuf.at[0, :, block_of(t)], 8))
    pieces.append((score.at[0, pl.ds(1, LAYERS - 1)], sbuf.at[pl.ds(1, LAYERS - 1)], 9))
    loads = [pltpu.make_async_copy(src, dst, sem_load.at[i]) for src, dst, i in pieces]
    for load in loads:
        load.start()

    for d in (1, 2, 3):
        pl.when(jnp.logical_or(wide, member + d < GROUP))(functools.partial(greet, at_group(d)))

    @pl.when(hub)
    def _():
        for d in (1, 2, 3):
            pl.when(jnp.logical_or(wide, at_x0 + d < LINE))(functools.partial(greet, at_x(d)))
        for m in range(GROUP):
            greet(at_other(m))

        for x in range(1, LINE):

            @pl.when(at_x0 < x)
            def _():
                for m in range(GROUP):
                    greet(((2 * x + 1) * GROUP + m, t))

    place = lax.broadcasted_iota(jnp.int32, (PARTS, PARTS * HERE), 1) - HERE * lax.broadcasted_iota(
        jnp.int32, (PARTS, PARTS * HERE), 0
    )
    pick = jnp.where(jnp.logical_and(place >= 0, place < HERE), F32(1.0), F32(0.0)).astype(BF16)

    def sum_layer(l):
        def body(i, carry):
            b, h = lax.div(i, 2), lax.rem(i, 2)
            blocks = [
                jnp.abs(dbuf[l, :, pl.ds(pl.multiple_of(i * HALF + j * LANES, LANES), LANES)]) for j in range(PARTS)
            ]
            sums[h, b, l] = jnp.dot(pick, jnp.concatenate(blocks, axis=0), preferred_element_type=F32)
            return carry

        lax.fori_loop(0, 2 * TASKS, body, 0, unroll=True)

    def mask_half(l, i):
        b, h = lax.div(i, 2), lax.rem(i, 2)
        own_limit = limit[0, l, expert]
        for j in range(PARTS):
            cols = pl.ds(pl.multiple_of(i * HALF + j * LANES, LANES), LANES)
            keep = sbuf[l, :, cols] < own_limit
            masked[b, l, h, :, j * LANES : (j + 1) * LANES] = jnp.where(
                keep, dbuf[l, :, cols].astype(F32), F32(0.0)
            ).astype(BF16)

    def mask_block(l, owner):
        def body(i, carry):
            mask_half(l, 2 * owner + i)
            return carry

        lax.fori_loop(0, 2, body, 0)

    def mask_layer(l):
        def body(i, carry):
            mask_half(l, i)
            return carry

        lax.fori_loop(0, 2 * TASKS, body, 0)

    def send_far(l):
        for h in range(2):
            send(masked.at[far_owner, l, h], far_in.at[h, l], FAR, ENTRIES, at_task(3 if h else 1))

    def send_near(l):
        for d, owner, h in ((1, up, 1), (3, down, 0)):
            send(masked.at[owner, l, h], raw_in.at[h, l], NEAR, ENTRIES, at_task(d))

    with jax.named_scope("load"):
        loads[0].wait()
        wait(sbuf.at[0, :, pl.ds(0, 3 * HALF)], sem_load.at[1])
    with jax.named_scope("mask0"):
        mask_block(0, far_owner)

    def all_sums():
        wait(dbuf.at[0, :, pl.ds(0, 4 * HALF)], sem_load.at[2])
        for l in range(LAYERS):
            wait(dbuf.at[l] if l else dbuf.at[0, :, pl.ds(0, 2 * HALF)], sem_load.at[3 + l])
            sum_layer(l)

    def mask_near():
        wait(sbuf.at[0, :, pl.ds(0, 4 * HALF)], sem_load.at[7])
        mask_block(0, up)
        mask_block(0, down)

    with jax.named_scope("sums0"):

        @pl.when(t < 2)
        def _():
            all_sums()
            mask_near()

    with jax.named_scope("bar"):
        met = jnp.where(wide, GROUP - 1, member) + 2 * late * (1 + at_x0) + jnp.where(hub, jnp.where(wide, GROUP - 1, at_x0), 0)
        pl.semaphore_wait(barrier, 2 + met)
    send_far(0)

    @pl.when(jnp.logical_not(wide))
    def _():
        for d in (1, 2, 3):
            for back, peer, sem in (
                (member - d >= 0, at_group(4 - d), sem_near),
                (jnp.logical_and(hub, at_x0 - d >= 0), at_x(4 - d), sem_line),
            ):

                @pl.when(back)
                def _():
                    pl.semaphore_signal(sem, inc=1, device_id=peer, device_id_type=MESH)

    with jax.named_scope("sums1"):

        @pl.when(t >= 2)
        def _():
            all_sums()
            mask_near()

    send_near(0)

    for l in range(LAYERS):
        whole = sums[0, 0, l] + sums[1, 0, l]
        for b in range(1, TASKS):
            whole = whole + sums[0, b, l] + sums[1, b, l]
        tot[l : l + 1, :] = jnp.sum(whole, axis=0, keepdims=True)
    tot[LAYERS:, :] = jnp.zeros((8 - LAYERS, LANES), F32)

    @pl.when(late == 1)
    def _():
        for m in (1, 3):
            send(tot, tot_l.at[member], TOTAL_L, TOTALS, at_other(m))

        for x in range(LINE - 1):

            @pl.when(at_x0 > x)
            def _():
                for m in (1, 3):
                    slot = GROUP * (at_x0 - x - 1) + member
                    send(tot, tot_f.at[slot], TOTAL_F, TOTALS, (2 * GROUP * x + m, t))

    with jax.named_scope("near"):

        to_come = GROUP - 1 - member

        @pl.when(jnp.logical_and(jnp.logical_not(wide), to_come > 0))
        def _():
            pl.semaphore_wait(sem_near, to_come)

    send(sums.at[1 - core], pair_in, PAIR, COLUMNS, at_group(1 - 2 * core + GROUP))

    @pl.when(late == 0)
    def _():
        for d in range(1, GROUP):
            pl.when(lax.rem(member + d, 2) == 1)(
                functools.partial(send, tot, tot_z.at[d - 1], TOTAL, TOTALS, at_group(d))
            )

    with jax.named_scope("masks"):
        wait(sbuf.at[0, :, pl.ds(0, 2 * HALF)], sem_load.at[8])
        mask_block(0, t)
        wait(sbuf.at[pl.ds(1, LAYERS - 1)], sem_load.at[9])
        for l in range(1, LAYERS):
            mask_layer(l)
            send_far(l)
        for l in range(1, LAYERS - HELD):
            send_near(l)

    with jax.named_scope("waitpair"):
        wait(pair_in, sem_got.at[PAIR])
    half[...] = sums[core] + pair_in[...]
    chip_out[...] = half[...]
    send(chip_out, chip_in, CHIP, COLUMNS, at_group(2))

    with jax.named_scope("totals1"):

        @pl.when(hub)
        def _():
            to_come_x = GROUP - 1 - at_x0

            @pl.when(jnp.logical_and(jnp.logical_not(wide), to_come_x > 0))
            def _():
                pl.semaphore_wait(sem_line, to_come_x)

            wait(tot_z, sem_got.at[TOTAL])
            early = tot[...] + tot_z[0] + tot_z[1] + tot_z[2]
            tot2[0] = early

            for d in (1, 2, 3):

                @pl.when(at_x0 + d >= LINE)
                def _():
                    send(tot2.at[0], tot_x.at[d - 1], TOTAL_X, TOTALS, at_x(d))

            wait(tot_l, sem_got.at[TOTAL_L])
            tot2[1] = early + tot_l[0] + tot_l[1] + tot_l[2] + tot_l[3]
            for d in (1, 2, 3):

                @pl.when(at_x0 + d < LINE)
                def _():
                    send(tot2.at[1], tot_x.at[d - 1], TOTAL_X, TOTALS, at_x(d))

    with jax.named_scope("waitchip"):
        wait(chip_in, sem_got.at[CHIP])
    half[...] = chip_out[...] + chip_in[...]
    send(half, half_in, WHOLE, COLUMNS, at_group(1 - 2 * core + GROUP))
    with jax.named_scope("totals2"):

        @pl.when(hub)
        def _():
            wait(tot_x, sem_got.at[TOTAL_X])
            grand[...] = tot2[1] + tot_x[0] + tot_x[1] + tot_x[2]

            for x in range(LINE - 1):

                @pl.when(at_x0 == x)
                def _():
                    count = GROUP * (LINE - 1 - x)
                    wait(tot_f.at[pl.ds(0, count)], sem_got.at[TOTAL_F])
                    whole = grand[...]
                    for i in range(count):
                        whole = whole + tot_f[i]
                    grand[...] = whole

            send(grand, grand, GRAND, TOTALS, at_other(GROUP - 1 - member))
            send(grand, grand, GRAND, TOTALS, at_other(GROUP - member))
            send(grand, grand, GRAND, TOTALS, at_group(GROUP - 1))

        @pl.when(jnp.logical_not(hub))
        def _():
            wait(grand, sem_got.at[GRAND])

    grand_mean = jnp.sum(grand[...], axis=1, keepdims=True) / F32(EXPERTS * ROWS * FF)
    with jax.named_scope("waitwhole"):
        wait(half_in, sem_got.at[WHOLE])

    def make_prob(b, l):
        mean_l = jnp.broadcast_to(grand_mean[l : l + 1, :], (PARTS, LANES))
        mine, theirs = half[b, l], half_in[b, l]
        for h in range(2):
            column = jnp.where(core == h, mine, theirs) / F32(ROWS)
            rounded = (0.2 + 0.7 * column / (column + mean_l)).astype(BF16)
            prob[b, l, h] = rounded
            inv_own[b, l, h] = 1.0 / rounded.astype(F32)

    def rescaled(block, tile, j):
        return block[:, j * LANES : (j + 1) * LANES].astype(F32) * tile[j : j + 1, :]

    with jax.named_scope("farprob"):
        for l in range(LAYERS):
            make_prob(far_owner, l)
        for h in range(2):
            send(prob.at[far_owner, :, h], far_prob.at[h], PROB_F, PROBS, at_task(3 if h else 1))
    with jax.named_scope("prob"):
        for owner in (up, down, t):
            for l in range(LAYERS):
                make_prob(owner, l)
    for l in range(LAYERS - HELD, LAYERS):
        send_near(l)
    for d, owner, h in ((1, up, 1), (3, down, 0)):
        pl.when(core == 1 - h)(
            functools.partial(send, prob.at[owner, :, h], prob_in.at[h], PROB_Y, PROBS, at_task(d))
        )

    with jax.named_scope("own"):
        for l in range(LAYERS):
            for h in range(2):
                tile = inv_own[t, l, h]
                for j in range(PARTS):
                    acc[l, h, :, j * LANES : (j + 1) * LANES] = rescaled(masked.at[t, l, h], tile, j)

    with jax.named_scope("waitfar"):
        wait(far_in, sem_got.at[FAR])
    with jax.named_scope("waitfarprob"):
        wait(far_prob, sem_got.at[PROB_F])
    for l in range(LAYERS):
        for h in range(2):
            owner = (up, down)[h]
            tile, far_tile = inv_own[owner, l, h], 1.0 / far_prob[h, l].astype(F32)
            for j in range(PARTS):
                joint[h, l, :, j * LANES : (j + 1) * LANES] = (
                    rescaled(masked.at[owner, l, h], tile, j) + rescaled(far_in.at[h, l], far_tile, j)
                ).astype(BF16)
            send(joint.at[h, l], joint_in.at[h, l], None, ENTRIES, at_task(3 if h else 1), sem_j.at[l])

    with jax.named_scope("waitpy"):
        mine = 1 - core
        wait(prob_in.at[mine], sem_got.at[PROB_Y])
        send(prob_in.at[mine], prob_in.at[mine], PROB_P, PROBS, at_group(1 - 2 * core + GROUP))
    with jax.named_scope("waitraw"):
        wait(raw_in, sem_got.at[NEAR])
    with jax.named_scope("waitpp"):
        wait(prob_in.at[core], sem_got.at[PROB_P])
    with jax.named_scope("raw"):
        for l in range(LAYERS):
            for h in range(2):
                tile = 1.0 / prob_in[h, l].astype(F32)
                for j in range(PARTS):
                    cols = slice(j * LANES, (j + 1) * LANES)
                    acc[l, h, :, cols] = acc[l, h, :, cols] + rescaled(raw_in.at[h, l], tile, j)
    for l in range(LAYERS):
        with jax.named_scope(f"waitjoint#l={l}"):
            wait(joint_in.at[:, l], sem_j.at[l])
        for h in range(2):
            for j in range(PARTS):
                cols = slice(j * LANES, (j + 1) * LANES)
                out[l, :, h * HALF + j * LANES : h * HALF + (j + 1) * LANES] = (
                    acc[l, h, :, cols] + joint_in[h, l, :, cols].astype(F32)
                ).astype(BF16)

    with jax.named_scope("waitsend"):
        @pl.when(hub)
        def _():
            wait(tot_f.at[pl.ds(0, 7)], sem_sent.at[TOTALS])

        for x in range(LINE):

            @pl.when(jnp.logical_and(late == 1, at_x0 == x))
            def _():
                wait(tot_f.at[pl.ds(0, 2 * (x + 1))], sem_sent.at[TOTALS])

        @pl.when(jnp.logical_and(late == 0, core == 0))
        def _():
            wait(tot_f.at[pl.ds(0, 2)], sem_sent.at[TOTALS])

        wait(masked.at[pl.ds(0, 3), 0], sem_sent.at[COLUMNS])
        wait(masked.at[0, 0, 0], sem_sent.at[PROBS])
        wait(masked.at[pl.ds(0, 3)], sem_sent.at[ENTRIES])


def on_device(task_deltas, rank_scores, keep_limits):
    dma = pltpu.SemaphoreType.DMA
    inputs = (pltpu.with_memory_space_constraint(x, pltpu.HBM) for x in (task_deltas, rank_scores, keep_limits))
    return pl.pallas_call(
        kernel,
        out_shape=jax.ShapeDtypeStruct((LAYERS, HERE, 2 * HALF), BF16),
        in_specs=[pl.BlockSpec(memory_space=pl.ANY)] * 3,
        out_specs=pl.BlockSpec(memory_space=pltpu.VMEM),
        scratch_shapes=[
            pltpu.SMEM((1, LAYERS, EXPERTS), jnp.int32),
            pltpu.VMEM((LAYERS, HERE, FF), BF16),
            pltpu.VMEM((LAYERS, HERE, FF), jnp.int32),
            pltpu.VMEM((TASKS, LAYERS, 2, HERE, HALF), BF16),
            pltpu.VMEM((2, TASKS, LAYERS, PARTS, LANES), F32),
            pltpu.VMEM((TASKS, LAYERS, PARTS, LANES), F32),
            *[pltpu.VMEM((TASKS, LAYERS, PARTS, LANES), F32)] * 4,
            pltpu.VMEM((TASKS, LAYERS, 2, PARTS, LANES), BF16),
            pltpu.VMEM((TASKS, LAYERS, 2, PARTS, LANES), F32),
            *[pltpu.VMEM((2, LAYERS, PARTS, LANES), BF16)] * 2,
            pltpu.VMEM((LAYERS, 2, HERE, HALF), F32),
            *[pltpu.VMEM((2, LAYERS, HERE, HALF), BF16)] * 4,
            pltpu.VMEM((8, LANES), F32),
            pltpu.VMEM((GROUP - 1, 8, LANES), F32),
            pltpu.VMEM((GROUP, 8, LANES), F32),
            pltpu.VMEM((2, 8, LANES), F32),
            pltpu.VMEM((3, 8, LANES), F32),
            pltpu.VMEM((3 * GROUP, 8, LANES), F32),
            pltpu.VMEM((8, LANES), F32),
            dma((10,)),
            dma((4,)),
            dma((13,)),
            dma((LAYERS,)),
            pltpu.SemaphoreType.REGULAR,
            pltpu.SemaphoreType.REGULAR,
        ],
        compiler_params=pltpu.CompilerParams(
            collective_id=0, has_side_effects=True, vmem_limit_bytes=32 * 1024 * 1024
        ),
    )(*inputs)


def solution(mesh):
    in_specs = (P("task", None, "shard", None), P("task", None, "shard", None), P("task", None, None))
    return jax.shard_map(on_device, mesh=mesh, in_specs=in_specs, out_specs=P(None, "shard", "task"), check_vma=False)
```

```python
import functools

import jax
import jax.numpy as jnp
from jax import lax
from jax.experimental import pallas as pl
from jax.experimental.pallas import tpu as pltpu
from jax.sharding import PartitionSpec as P

EXPERTS = 8
ROWS = 64
FF = 16384
LAYERS = 4
TASKS = 4
SHARDS = 32
GROUP = 4
LINE = 4
HERE = 16
HALF = 2048
LANES = 128
PARTS = HALF // LANES
HELD = 1

MESH = pl.DeviceIdType.MESH
F32 = jnp.float32
BF16 = jnp.bfloat16


def kernel(
    delta, score, limit_in, out,
    limit, dbuf, sbuf, masked, sums, pair_in, chip_out, chip_in, half, half_in, prob, inv_own, prob_in, far_prob, acc, raw_in,
    far_in, joint, joint_in, tot, tot_z, tot_l, tot2, tot_x, tot_f, grand,
    sem_load, sem_sent, sem_got, sem_j, sem_near, sem_line,
):
    s, t = lax.axis_index("shard"), lax.axis_index("task")
    expert = lax.div(s, GROUP)
    member = lax.rem(s, GROUP)
    core = lax.rem(s, 2)
    first = expert * GROUP
    late = lax.rem(expert, 2)
    other = (expert + 1 - 2 * late) * GROUP
    hub = jnp.logical_and(late == 0, core == 1)

    def at_task(d):
        return (s, lax.rem(t + d, TASKS))

    def at_x(d):
        return (lax.rem(s + 2 * GROUP * d, SHARDS), t)

    def at_other(m):
        return (other + m, t)

    def block_of(owner):
        return pl.ds(pl.multiple_of(owner * 2 * HALF, 2 * HALF), 2 * HALF)

    def at_group(d):
        return (first + lax.rem(member + d, GROUP), t)

    def send(src, dst, kind, sent, to, got=None):
        copy = pltpu.make_async_remote_copy(
            src_ref=src, dst_ref=dst, send_sem=sem_sent.at[sent], recv_sem=sem_got.at[kind] if got is None else got,
            device_id=to, device_id_type=MESH,
        )
        copy.start()

    def wait(ref, sem):
        pltpu.make_async_copy(ref, ref, sem).wait()

    PAIR, CHIP, WHOLE, TOTAL, TOTAL_L, TOTAL_X, TOTAL_F, GRAND, PROB_F, PROB_Y, PROB_P, NEAR, FAR = range(13)
    COLUMNS, TOTALS, PROBS, ENTRIES = range(4)

    barrier = pltpu.get_barrier_semaphore()

    def greet(to):
        pl.semaphore_signal(barrier, inc=1, device_id=to, device_id_type=MESH)

    wide = t < 2
    at_x0 = lax.div(s, 2 * GROUP)
    greet(at_task(1))
    greet(at_task(3))
    up, down, far_owner = lax.rem(t + 1, TASKS), lax.rem(t + 3, TASKS), lax.rem(t + 2, TASKS)
    first_d, first_s = delta.at[0, 0], score.at[0, 0]
    pieces = [(limit_in, limit, 0)]
    pieces.append((first_d.at[:, block_of(far_owner)], dbuf.at[0, :, block_of(far_owner)], 1))
    pieces.append((first_s.at[:, block_of(far_owner)], sbuf.at[0, :, block_of(far_owner)], 1))
    for owner in (up, down):
        pieces.append((first_d.at[:, block_of(owner)], dbuf.at[0, :, block_of(owner)], 2))
    pieces.append((first_d.at[:, block_of(t)], dbuf.at[0, :, block_of(t)], 3))
    for l in range(1, LAYERS):
        pieces.append((delta.at[0, l], dbuf.at[l], 3 + l))
    for owner in (up, down):
        pieces.append((first_s.at[:, block_of(owner)], sbuf.at[0, :, block_of(owner)], 7))
    pieces.append((first_s.at[:, block_of(t)], sbuf.at[0, :, block_of(t)], 8))
    pieces.append((score.at[0, pl.ds(1, LAYERS - 1)], sbuf.at[pl.ds(1, LAYERS - 1)], 9))
    loads = [pltpu.make_async_copy(src, dst, sem_load.at[i]) for src, dst, i in pieces]
    for load in loads:
        load.start()

    for d in (1, 2, 3):
        pl.when(jnp.logical_or(wide, member + d < GROUP))(functools.partial(greet, at_group(d)))

    @pl.when(hub)
    def _():
        for d in (1, 2, 3):
            pl.when(jnp.logical_or(wide, at_x0 + d < LINE))(functools.partial(greet, at_x(d)))
        for m in range(GROUP):
            greet(at_other(m))

        for x in range(1, LINE):

            @pl.when(at_x0 < x)
            def _():
                for m in range(GROUP):
                    greet(((2 * x + 1) * GROUP + m, t))

    place = lax.broadcasted_iota(jnp.int32, (PARTS, PARTS * HERE), 1) - HERE * lax.broadcasted_iota(
        jnp.int32, (PARTS, PARTS * HERE), 0
    )
    pick = jnp.where(jnp.logical_and(place >= 0, place < HERE), F32(1.0), F32(0.0)).astype(BF16)

    def sum_layer(l):
        def body(i, carry):
            b, h = lax.div(i, 2), lax.rem(i, 2)
            blocks = [
                jnp.abs(dbuf[l, :, pl.ds(pl.multiple_of(i * HALF + j * LANES, LANES), LANES)]) for j in range(PARTS)
            ]
            sums[h, b, l] = jnp.dot(pick, jnp.concatenate(blocks, axis=0), preferred_element_type=F32)
            return carry

        lax.fori_loop(0, 2 * TASKS, body, 0, unroll=True)

    def mask_half(l, i):
        b, h = lax.div(i, 2), lax.rem(i, 2)
        own_limit = limit[0, l, expert]
        for j in range(PARTS):
            cols = pl.ds(pl.multiple_of(i * HALF + j * LANES, LANES), LANES)
            keep = sbuf[l, :, cols] < own_limit
            masked[b, l, h, :, j * LANES : (j + 1) * LANES] = jnp.where(
                keep, dbuf[l, :, cols].astype(F32), F32(0.0)
            ).astype(BF16)

    def mask_block(l, owner):
        def body(i, carry):
            mask_half(l, 2 * owner + i)
            return carry

        lax.fori_loop(0, 2, body, 0)

    def mask_layer(l):
        def body(i, carry):
            mask_half(l, i)
            return carry

        lax.fori_loop(0, 2 * TASKS, body, 0)

    def send_far(l):
        for h in range(2):
            send(masked.at[far_owner, l, h], far_in.at[h, l], FAR, ENTRIES, at_task(3 if h else 1))

    def send_near(l):
        for d, owner, h in ((1, up, 1), (3, down, 0)):
            send(masked.at[owner, l, h], raw_in.at[h, l], NEAR, ENTRIES, at_task(d))

    with jax.named_scope("load"):
        loads[0].wait()
        wait(sbuf.at[0, :, pl.ds(0, 3 * HALF)], sem_load.at[1])
    with jax.named_scope("mask0"):
        mask_block(0, far_owner)

    def all_sums():
        wait(dbuf.at[0, :, pl.ds(0, 4 * HALF)], sem_load.at[2])
        for l in range(LAYERS):
            wait(dbuf.at[l] if l else dbuf.at[0, :, pl.ds(0, 2 * HALF)], sem_load.at[3 + l])
            sum_layer(l)

    def mask_near():
        wait(sbuf.at[0, :, pl.ds(0, 4 * HALF)], sem_load.at[7])
        mask_block(0, up)
        mask_block(0, down)

    with jax.named_scope("sums0"):

        @pl.when(t < 2)
        def _():
            all_sums()
            mask_near()

    with jax.named_scope("bar"):
        met = jnp.where(wide, GROUP - 1, member) + 2 * late * (1 + at_x0) + jnp.where(hub, jnp.where(wide, GROUP - 1, at_x0), 0)
        pl.semaphore_wait(barrier, 2 + met)
    send_far(0)

    @pl.when(jnp.logical_not(wide))
    def _():
        for d in (1, 2, 3):
            for back, peer, sem in (
                (member - d >= 0, at_group(4 - d), sem_near),
                (jnp.logical_and(hub, at_x0 - d >= 0), at_x(4 - d), sem_line),
            ):

                @pl.when(back)
                def _():
                    pl.semaphore_signal(sem, inc=1, device_id=peer, device_id_type=MESH)

    with jax.named_scope("sums1"):

        @pl.when(t >= 2)
        def _():
            all_sums()
            mask_near()

    send_near(0)

    for l in range(LAYERS):
        whole = sums[0, 0, l] + sums[1, 0, l]
        for b in range(1, TASKS):
            whole = whole + sums[0, b, l] + sums[1, b, l]
        tot[l : l + 1, :] = jnp.sum(whole, axis=0, keepdims=True)
    tot[LAYERS:, :] = jnp.zeros((8 - LAYERS, LANES), F32)

    @pl.when(late == 1)
    def _():
        for m in (1, 3):
            send(tot, tot_l.at[member], TOTAL_L, TOTALS, at_other(m))

        for x in range(LINE - 1):

            @pl.when(at_x0 > x)
            def _():
                for m in (1, 3):
                    slot = GROUP * (at_x0 - x - 1) + member
                    send(tot, tot_f.at[slot], TOTAL_F, TOTALS, (2 * GROUP * x + m, t))

    with jax.named_scope("near"):

        to_come = GROUP - 1 - member

        @pl.when(jnp.logical_and(jnp.logical_not(wide), to_come > 0))
        def _():
            pl.semaphore_wait(sem_near, to_come)

    send(sums.at[1 - core], pair_in, PAIR, COLUMNS, at_group(1 - 2 * core + GROUP))

    @pl.when(late == 0)
    def _():
        for d in range(1, GROUP):
            pl.when(lax.rem(member + d, 2) == 1)(
                functools.partial(send, tot, tot_z.at[d - 1], TOTAL, TOTALS, at_group(d))
            )

    with jax.named_scope("masks"):
        wait(sbuf.at[0, :, pl.ds(0, 2 * HALF)], sem_load.at[8])
        mask_block(0, t)
        wait(sbuf.at[pl.ds(1, LAYERS - 1)], sem_load.at[9])
        for l in range(1, LAYERS):
            mask_layer(l)
            send_far(l)
        for l in range(1, LAYERS - HELD):
            send_near(l)

    with jax.named_scope("waitpair"):
        wait(pair_in, sem_got.at[PAIR])
    half[...] = sums[core] + pair_in[...]
    chip_out[...] = half[...].astype(BF16)
    send(chip_out, chip_in, CHIP, COLUMNS, at_group(2))

    with jax.named_scope("totals1"):

        @pl.when(hub)
        def _():
            to_come_x = GROUP - 1 - at_x0

            @pl.when(jnp.logical_and(jnp.logical_not(wide), to_come_x > 0))
            def _():
                pl.semaphore_wait(sem_line, to_come_x)

            wait(tot_z, sem_got.at[TOTAL])
            early = tot[...] + tot_z[0] + tot_z[1] + tot_z[2]
            tot2[0] = early

            for d in (1, 2, 3):

                @pl.when(at_x0 + d >= LINE)
                def _():
                    send(tot2.at[0], tot_x.at[d - 1], TOTAL_X, TOTALS, at_x(d))

            wait(tot_l, sem_got.at[TOTAL_L])
            tot2[1] = early + tot_l[0] + tot_l[1] + tot_l[2] + tot_l[3]
            for d in (1, 2, 3):

                @pl.when(at_x0 + d < LINE)
                def _():
                    send(tot2.at[1], tot_x.at[d - 1], TOTAL_X, TOTALS, at_x(d))

    with jax.named_scope("waitchip"):
        wait(chip_in, sem_got.at[CHIP])
    half[...] = half[...] + chip_in[...].astype(F32)
    send(half, half_in, WHOLE, COLUMNS, at_group(1 - 2 * core + GROUP))
    with jax.named_scope("totals2"):

        @pl.when(hub)
        def _():
            wait(tot_x, sem_got.at[TOTAL_X])
            grand[...] = tot2[1] + tot_x[0] + tot_x[1] + tot_x[2]

            for x in range(LINE - 1):

                @pl.when(at_x0 == x)
                def _():
                    count = GROUP * (LINE - 1 - x)
                    wait(tot_f.at[pl.ds(0, count)], sem_got.at[TOTAL_F])
                    whole = grand[...]
                    for i in range(count):
                        whole = whole + tot_f[i]
                    grand[...] = whole

            send(grand, grand, GRAND, TOTALS, at_other(GROUP - 1 - member))
            send(grand, grand, GRAND, TOTALS, at_other(GROUP - member))
            send(grand, grand, GRAND, TOTALS, at_group(GROUP - 1))

        @pl.when(jnp.logical_not(hub))
        def _():
            wait(grand, sem_got.at[GRAND])

    grand_mean = jnp.sum(grand[...], axis=1, keepdims=True) / F32(EXPERTS * ROWS * FF)
    with jax.named_scope("waitwhole"):
        wait(half_in, sem_got.at[WHOLE])

    def make_prob(b, l):
        mean_l = jnp.broadcast_to(grand_mean[l : l + 1, :], (PARTS, LANES))
        mine, theirs = half[b, l], half_in[b, l]
        for h in range(2):
            column = jnp.where(core == h, mine, theirs) / F32(ROWS)
            rounded = (0.2 + 0.7 * column / (column + mean_l)).astype(BF16)
            prob[b, l, h] = rounded
            inv_own[b, l, h] = 1.0 / rounded.astype(F32)

    def rescaled(block, tile, j):
        return block[:, j * LANES : (j + 1) * LANES].astype(F32) * tile[j : j + 1, :]

    with jax.named_scope("farprob"):
        for l in range(LAYERS):
            make_prob(far_owner, l)
        for h in range(2):
            send(prob.at[far_owner, :, h], far_prob.at[h], PROB_F, PROBS, at_task(3 if h else 1))
    with jax.named_scope("prob"):
        for owner in (up, down, t):
            for l in range(LAYERS):
                make_prob(owner, l)
    for l in range(LAYERS - HELD, LAYERS):
        send_near(l)
    for d, owner, h in ((1, up, 1), (3, down, 0)):
        pl.when(core == 1 - h)(
            functools.partial(send, prob.at[owner, :, h], prob_in.at[h], PROB_Y, PROBS, at_task(d))
        )

    with jax.named_scope("own"):
        for l in range(LAYERS):
            for h in range(2):
                tile = inv_own[t, l, h]
                for j in range(PARTS):
                    acc[l, h, :, j * LANES : (j + 1) * LANES] = rescaled(masked.at[t, l, h], tile, j)

    with jax.named_scope("waitfar"):
        wait(far_in, sem_got.at[FAR])
    with jax.named_scope("waitfarprob"):
        wait(far_prob, sem_got.at[PROB_F])
    for l in range(LAYERS):
        for h in range(2):
            owner = (up, down)[h]
            tile, far_tile = inv_own[owner, l, h], 1.0 / far_prob[h, l].astype(F32)
            for j in range(PARTS):
                joint[h, l, :, j * LANES : (j + 1) * LANES] = (
                    rescaled(masked.at[owner, l, h], tile, j) + rescaled(far_in.at[h, l], far_tile, j)
                ).astype(BF16)
            send(joint.at[h, l], joint_in.at[h, l], None, ENTRIES, at_task(3 if h else 1), sem_j.at[l])

    with jax.named_scope("waitpy"):
        mine = 1 - core
        wait(prob_in.at[mine], sem_got.at[PROB_Y])
        send(prob_in.at[mine], prob_in.at[mine], PROB_P, PROBS, at_group(1 - 2 * core + GROUP))
    with jax.named_scope("waitraw"):
        wait(raw_in, sem_got.at[NEAR])
    with jax.named_scope("waitpp"):
        wait(prob_in.at[core], sem_got.at[PROB_P])
    with jax.named_scope("raw"):
        for l in range(LAYERS):
            for h in range(2):
                tile = 1.0 / prob_in[h, l].astype(F32)
                for j in range(PARTS):
                    cols = slice(j * LANES, (j + 1) * LANES)
                    acc[l, h, :, cols] = acc[l, h, :, cols] + rescaled(raw_in.at[h, l], tile, j)
    for l in range(LAYERS):
        with jax.named_scope(f"waitjoint#l={l}"):
            wait(joint_in.at[:, l], sem_j.at[l])
        for h in range(2):
            for j in range(PARTS):
                cols = slice(j * LANES, (j + 1) * LANES)
                out[l, :, h * HALF + j * LANES : h * HALF + (j + 1) * LANES] = (
                    acc[l, h, :, cols] + joint_in[h, l, :, cols].astype(F32)
                ).astype(BF16)

    with jax.named_scope("waitsend"):
        @pl.when(hub)
        def _():
            wait(tot_f.at[pl.ds(0, 7)], sem_sent.at[TOTALS])

        for x in range(LINE):

            @pl.when(jnp.logical_and(late == 1, at_x0 == x))
            def _():
                wait(tot_f.at[pl.ds(0, 2 * (x + 1))], sem_sent.at[TOTALS])

        @pl.when(jnp.logical_and(late == 0, core == 0))
        def _():
            wait(tot_f.at[pl.ds(0, 2)], sem_sent.at[TOTALS])

        wait(dbuf.at[0, :, pl.ds(0, 5 * HALF)], sem_sent.at[COLUMNS])
        wait(masked.at[0, 0, 0], sem_sent.at[PROBS])
        wait(masked.at[pl.ds(0, 3)], sem_sent.at[ENTRIES])


def on_device(task_deltas, rank_scores, keep_limits):
    dma = pltpu.SemaphoreType.DMA
    inputs = (pltpu.with_memory_space_constraint(x, pltpu.HBM) for x in (task_deltas, rank_scores, keep_limits))
    return pl.pallas_call(
        kernel,
        out_shape=jax.ShapeDtypeStruct((LAYERS, HERE, 2 * HALF), BF16),
        in_specs=[pl.BlockSpec(memory_space=pl.ANY)] * 3,
        out_specs=pl.BlockSpec(memory_space=pltpu.VMEM),
        scratch_shapes=[
            pltpu.SMEM((1, LAYERS, EXPERTS), jnp.int32),
            pltpu.VMEM((LAYERS, HERE, FF), BF16),
            pltpu.VMEM((LAYERS, HERE, FF), jnp.int32),
            pltpu.VMEM((TASKS, LAYERS, 2, HERE, HALF), BF16),
            pltpu.VMEM((2, TASKS, LAYERS, PARTS, LANES), F32),
            pltpu.VMEM((TASKS, LAYERS, PARTS, LANES), F32),
            *[pltpu.VMEM((TASKS, LAYERS, PARTS, LANES), BF16)] * 2,
            *[pltpu.VMEM((TASKS, LAYERS, PARTS, LANES), F32)] * 2,
            pltpu.VMEM((TASKS, LAYERS, 2, PARTS, LANES), BF16),
            pltpu.VMEM((TASKS, LAYERS, 2, PARTS, LANES), F32),
            *[pltpu.VMEM((2, LAYERS, PARTS, LANES), BF16)] * 2,
            pltpu.VMEM((LAYERS, 2, HERE, HALF), F32),
            *[pltpu.VMEM((2, LAYERS, HERE, HALF), BF16)] * 4,
            pltpu.VMEM((8, LANES), F32),
            pltpu.VMEM((GROUP - 1, 8, LANES), F32),
            pltpu.VMEM((GROUP, 8, LANES), F32),
            pltpu.VMEM((2, 8, LANES), F32),
            pltpu.VMEM((3, 8, LANES), F32),
            pltpu.VMEM((3 * GROUP, 8, LANES), F32),
            pltpu.VMEM((8, LANES), F32),
            dma((10,)),
            dma((4,)),
            dma((13,)),
            dma((LAYERS,)),
            pltpu.SemaphoreType.REGULAR,
            pltpu.SemaphoreType.REGULAR,
        ],
        compiler_params=pltpu.CompilerParams(
            collective_id=0, has_side_effects=True, vmem_limit_bytes=32 * 1024 * 1024
        ),
    )(*inputs)


def solution(mesh):
    in_specs = (P("task", None, "shard", None), P("task", None, "shard", None), P("task", None, None))
    return jax.shard_map(on_device, mesh=mesh, in_specs=in_specs, out_specs=P(None, "shard", "task"), check_vma=False)
```
